128 devices in a mesh: dp: 8 (over x, core), tensor: 16 (over z, y).
Axes of the slice: x: 4, y: 4, z: 4, core: 2. Of those that a mesh axis runs over, the one named last changes fastest.
Arguments:
- activations: bfloat16 [4096, 28672], P('dp', 'tensor'), parts along dimension 0, may hold values from -6 to 6
- down_weight: bfloat16 [28672, 6144], P('tensor'), may hold values from -0.046875 to 0.046875
Outputs:
- projected: bfloat16 [4096, 6144], P(('dp', 'tensor')), parts along dimension 0
The draws below stay inside these ranges and needn't reach their ends.
There are 8 independent parts, one for each index of `dp`. The reference program is written for one: setup_inputs(seed, part) draws one part's arguments, and reference() takes and returns one part's arrays. A program takes and returns all parts, laid end to end along the dimension named above; an argument that names none is the same for every part. Nothing has to cross between parts.
All inputs are finite; a program needn't handle non-finite values.
Results may differ from the reference program's by a relative error of at most 0.015.
Values may be sent and summed in bfloat16 or wider, within the bound.
A program may use at most 128 MiB of HBM per device.

```python
import math
import jax
import jax.numpy as jnp
import numpy as np
from jax import lax

SYL = 1024
FF = 28672
DW = 6144
TOK = 512


def with_spikes(result, stream_key, source, target, blocks, factor):
    def block_of(position):
        return (jnp.arange(result.shape[position]) // (result.shape[position] // blocks)).reshape((-1,) + (1,) * (result.ndim - 1 - position))

    near = jax.random.permutation(stream_key, blocks)[block_of(target)]
    far = (block_of(target) + blocks // 2) % blocks
    return jnp.where((block_of(source) == near) | (block_of(source) == far), factor * result, result)


def level_of(stream_key, extent, cuts, smallest, top_value):
    loudness, own = 1.0, jax.random.fold_in(stream_key, 6)
    for position, parts in cuts:
        draws = jnp.exp(jax.random.uniform(jax.random.fold_in(own, position), (parts,), jnp.float32, smallest / len(cuts), top_value / len(cuts)))
        loudness = loudness * jnp.repeat(draws, extent[position] // parts).reshape([-1 if axis == position else 1 for axis in range(len(extent))])
    return loudness


def normal_values(own_key, dims, scale, limit, cuts=(), held_as=jnp.bfloat16):
    gain = level_of(own_key, dims, cuts, -0.22, 0.18) if cuts else 1.0
    values = jax.random.normal(own_key, dims, jnp.float32) * scale * gain
    return jnp.minimum(jnp.maximum(values, -limit), limit).astype(held_as)


def noise_with(own_key, extent, scale, reach, shards, heavy, dtype=jnp.bfloat16):
    result = scale * jax.random.normal(own_key, extent, jnp.float32)
    if shards:
        result = result * level_of(own_key, extent, shards, -0.22, 0.18)
    return jnp.clip(with_spikes(result, jax.random.fold_in(own_key, 3), *heavy), -reach, reach).astype(dtype)


def setup_inputs(seed: int = 0, part: int = 0) -> dict:
    arg_keys = jax.random.split(jax.random.key(seed), 3)
    own_keys = jax.random.split(jax.random.fold_in(arg_keys[2], part), 3)
    return {
        "activations": normal_values(own_keys[0], (TOK, FF), 1.0, 6.0, ((1, 16),)),
        "down_weight": noise_with(arg_keys[1], (FF, DW), FF ** -0.5, 0.046875, ((0, 16),), (0, 1, 16, 2.0)),
    }


def paley_matrix():
    modulus = 13
    residues = set((value * value % modulus for value in range(1, modulus)))
    jacobsthal = np.array([[0.0 if row_at == col_at else 1.0 if (col_at - row_at) % modulus in residues else -1.0 for col_at in range(modulus)] for row_at in range(modulus)])
    confer = np.zeros((14, 14))
    confer[0, 1:] = 1.0
    confer[1:, 0] = 1.0
    confer[1:, 1:] = jacobsthal
    return np.kron(confer, np.array([[1.0, 1.0], [1.0, -1.0]])) + np.kron(np.eye(14), np.array([[1.0, -1.0], [-1.0, -1.0]]))

def sylvester(order):
    matrix = np.ones((1, 1))
    while matrix.shape[0] < order:
        matrix = np.kron(matrix, np.array([[1.0, 1.0], [1.0, -1.0]]))
    return matrix

def quantize(rotated, largest):
    token_scale = jnp.maximum(largest, 1.0)
    levels = 7.0 * rotated / token_scale
    snapped = levels - jnp.sin(2.0 * math.pi * levels) / (2.0 * math.pi)
    return (snapped * token_scale / 7.0).astype(jnp.bfloat16)

def reference(activations, down_weight):
    count_rows = activations.shape[0]
    small_table = jnp.asarray(paley_matrix(), jnp.float32)
    power_table = jnp.asarray(sylvester(SYL), jnp.float32)
    values = activations.astype(jnp.float32).reshape(count_rows * SYL, 28)
    inner = jnp.dot(values, small_table, precision=lax.Precision.HIGHEST).reshape(count_rows, SYL, 28)
    outer = jnp.einsum('tji,jk->tki', inner, power_table, precision=lax.Precision.HIGHEST)
    rotated = outer.reshape(count_rows, FF) * (1.0 / math.sqrt(FF))
    largest = lax.optimization_barrier(jnp.max(jnp.abs(rotated), axis=1, keepdims=True))
    dequant = quantize(rotated, largest)
    return jnp.dot(dequant, down_weight, preferred_element_type=jnp.float32).astype(jnp.bfloat16)
```

```python
import functools
import math

import jax
import jax.numpy as jnp
import numpy as np
from jax import lax
from jax.experimental import pallas as pl
from jax.experimental.pallas import tpu as pltpu
from jax.sharding import PartitionSpec as P

MESH = pl.DeviceIdType.MESH
CHUNKS = 2
ROWS = 16
PIECES = 3
WIDE = 1024
TILE = 256
OFFSETS = (
    (0, 1), (1, 0), (0, 3), (3, 0), (1, 1), (3, 3), (1, 3), (3, 1),
    (0, 2), (2, 0), (1, 2), (2, 1), (3, 2), (2, 3), (2, 2),
)


def paley_matrix():
    modulus = 13
    residues = set((value * value % modulus for value in range(1, modulus)))
    confer = np.zeros((14, 14))
    confer[0, 1:] = 1.0
    confer[1:, 0] = 1.0
    for row in range(modulus):
        for col in range(modulus):
            if row != col:
                confer[1 + row, 1 + col] = 1.0 if (col - row) % modulus in residues else -1.0
    return np.kron(confer, np.array([[1.0, 1.0], [1.0, -1.0]])) + np.kron(
        np.eye(14), np.array([[1.0, -1.0], [-1.0, -1.0]])
    )


def sylvester(order):
    matrix = np.ones((1, 1))
    while matrix.shape[0] < order:
        matrix = np.kron(matrix, np.array([[1.0, 1.0], [1.0, -1.0]]))
    return matrix


def sine_coefficients():
    nodes = np.cos(np.pi * (np.arange(64) + 0.5) / 64)
    r2 = 0.125 + 0.125 * nodes
    root = np.sqrt(r2)
    target = np.sinc(2 * root)
    return np.polynomial.chebyshev.Chebyshev.fit(r2, target, 6, domain=[0, 0.25]).convert(
        kind=np.polynomial.Polynomial
    ).coef


SINE = [float(c) for c in sine_coefficients()]


def kernel(
    a_hbm, r_hbm, w_hbm, o_hbm,
    a_in, table, weight, mixed, gathered, rotated, quant, dequant,
    part, far, near, summed, far2, near2, result,
    in_sem, w_sem, send_a, recv_a, send_q, recv_q,
    send1, send2, recv_far, recv_near, recv_far2, recv_near2, out_sem,
):
    me = lax.axis_index("tensor")
    z, y = me // 4, me % 4
    width = a_hbm.shape[-1]
    half = width // 2
    norm = 1.0 / math.sqrt(width * 16)

    def partner(offset):
        return ((z + offset[0]) % 4) * 4 + (y + offset[1]) % 4

    loads = [
        pltpu.make_async_copy(a_hbm.at[:, pl.ds(ROWS * c, ROWS)], a_in.at[c], in_sem.at[c])
        for c in range(CHUNKS)
    ]
    table_load = pltpu.make_async_copy(r_hbm, table, in_sem.at[CHUNKS])
    loads[0].start()
    table_load.start()
    for c in range(1, CHUNKS):
        loads[c].start()
    w_loads = [
        pltpu.make_async_copy(w_hbm.at[:, pl.ds(WIDE * i, WIDE)], weight.at[i], w_sem.at[i])
        for i in range(2 * PIECES)
    ]

    barrier = pltpu.get_barrier_semaphore()
    for offset in OFFSETS:
        pl.semaphore_signal(
            barrier, inc=1, device_id={"tensor": partner(offset)}, device_id_type=MESH
        )

    def rotate(c):
        left = a_in[c, :, :, 0:half].reshape(16 * ROWS, half)
        right = a_in[c, :, :, half:width].reshape(16 * ROWS, half)
        for at in range(0, half, TILE):
            size = min(TILE, half - at)
            cols = table[:, at : at + size]
            first = jnp.dot(left, cols, preferred_element_type=jnp.float32)
            second = jnp.dot(right, cols, preferred_element_type=jnp.float32)
            mixed[c, :, :, at : at + size] = (
                (first + second).astype(jnp.bfloat16).reshape(16, ROWS, size)
            )
            mixed[c, :, :, half + at : half + at + size] = (
                (first - second).astype(jnp.bfloat16).reshape(16, ROWS, size)
            )

    def exchange(c, source, target, send, recv):
        for offset in OFFSETS:
            e = partner(offset)
            pltpu.make_async_remote_copy(
                src_ref=source.at[c, e],
                dst_ref=target.at[c, me],
                send_sem=send.at[c],
                recv_sem=recv.at[c],
                device_id={"tensor": e},
                device_id_type=MESH,
            ).start()
        target[c, me] = source[c, me]

    def exchange_all(c, source, target, send, recv):
        return pltpu.make_async_remote_copy(
            src_ref=source.at[c, pl.ds(0, 15)],
            dst_ref=target.at[c, pl.ds(0, 15)],
            send_sem=send.at[c],
            recv_sem=recv.at[c],
            device_id={"tensor": partner((0, 1))},
            device_id_type=MESH,
        )

    def transform(c):
        def butterfly(t, largest):
            cols = pl.ds(pl.multiple_of(t * 128, 128), 128)
            v = [gathered[c, e, :, cols].astype(jnp.float32) for e in range(16)]
            for bit in (1, 2, 4, 8):
                n = list(v)
                for e in range(16):
                    n[e] = v[e ^ bit] - v[e] if e & bit else v[e] + v[e ^ bit]
                v = n
            for e in range(16):
                rotated[e, :, cols] = v[e]
            m = [jnp.abs(x) for x in v]
            while len(m) > 1:
                m = [jnp.maximum(m[i], m[i + 1]) for i in range(0, len(m), 2)]
            return jnp.maximum(largest, m[0])

        largest = lax.fori_loop(
            0, width // 128, butterfly, jnp.zeros((ROWS, 128), jnp.float32)
        )
        scale = jnp.maximum(jnp.max(largest, axis=1, keepdims=True) * norm, 1.0)
        up = jnp.broadcast_to(7.0 * norm / scale, (ROWS, 128))
        down = jnp.broadcast_to(scale / 7.0, (ROWS, 128))

        def staircase(t, carry):
            cols = pl.ds(pl.multiple_of(t * 128, 128), 128)
            for e in range(16):
                levels = rotated[e, :, cols] * up
                r = levels - jnp.round(levels)
                r2 = r * r
                series = jnp.full_like(r2, SINE[-1])
                for coefficient in SINE[-2::-1]:
                    series = series * r2 + coefficient
                quant[c, e, :, cols] = ((levels - r * series) * down).astype(jnp.bfloat16)
            return carry

        lax.fori_loop(0, width // 128, staircase, 0)

    def axes(h):
        along_y = [partner((0, 1)), partner((0, 3))]
        along_z = [partner((1, 0)), partner((3, 0))]
        return (y, z, along_y, along_z) if h == 0 else (z, y, along_z, along_y)

    def send(source, target, s, r, e):
        pltpu.make_async_remote_copy(
            src_ref=source, dst_ref=target, send_sem=s, recv_sem=r,
            device_id={"tensor": e}, device_id_type=MESH,
        ).start()

    order = [(c, p, h) for c in range(CHUNKS) for p in range(PIECES) for h in range(2)]

    def project(g):
        c, p, h = order[g]
        i = h * PIECES + p
        if c == 0:
            w_loads[i].wait()

        def tile(n, carry):
            cols = pl.ds(pl.multiple_of(n * TILE, TILE), TILE)
            product = jnp.dot(
                dequant[c].reshape(16 * ROWS, width),
                weight[i, :, cols],
                preferred_element_type=jnp.float32,
            ).astype(jnp.bfloat16)
            for e in range(16):
                u, v = (e % 4, e // 4) if h == 0 else (e // 4, e % 4)
                part[g, u, v, :, cols] = product[e * ROWS : (e + 1) * ROWS]
            return carry

        lax.fori_loop(0, WIDE // TILE, tile, 0)
        u, v, first, second = axes(h)
        up, down, opposite = (u + 1) % 4, (u + 3) % 4, (u + 2) % 4
        low, high = pl.ds(0, 2), pl.ds(2, 2)
        send(part.at[g, opposite, low], far.at[g, 0], send1.at[g], recv_far.at[g], first[0])
        send(part.at[g, opposite, high], far.at[g, 1], send1.at[g], recv_far.at[g], first[1])
        send(part.at[g, up, high], near.at[g, 0, high], send1.at[g], recv_near.at[g], first[0])
        send(part.at[g, down, low], near.at[g, 1, low], send1.at[g], recv_near.at[g], first[1])

    def fake(source, target, s, r):
        return pltpu.make_async_remote_copy(
            src_ref=source, dst_ref=target, send_sem=s, recv_sem=r,
            device_id={"tensor": partner((0, 1))}, device_id_type=MESH,
        )

    def relay(g):
        c, p, h = order[g]
        u, v, first, second = axes(h)
        up, down = (u + 1) % 4, (u + 3) % 4
        fake(far.at[g], far.at[g], send1.at[g], recv_far.at[g]).wait_recv()
        for k in range(2):
            part[g, up, k] = (
                part[g, up, k].astype(jnp.float32) + far[g, 0, k].astype(jnp.float32)
            ).astype(jnp.bfloat16)
            part[g, down, 2 + k] = (
                part[g, down, 2 + k].astype(jnp.float32) + far[g, 1, k].astype(jnp.float32)
            ).astype(jnp.bfloat16)
        low, high = pl.ds(0, 2), pl.ds(2, 2)
        send(part.at[g, up, low], near.at[g, 0, low], send1.at[g], recv_near.at[g], first[0])
        send(part.at[g, down, high], near.at[g, 1, high], send1.at[g], recv_near.at[g], first[1])

    def gather(g):
        c, p, h = order[g]
        u, v, first, second = axes(h)
        fake(near.at[g], near.at[g], send1.at[g], recv_near.at[g]).wait_recv()
        for k in range(4):
            summed[g, k] = (
                part[g, u, k].astype(jnp.float32)
                + near[g, 0, k].astype(jnp.float32)
                + near[g, 1, k].astype(jnp.float32)
            ).astype(jnp.bfloat16)
        up, down, opposite = (v + 1) % 4, (v + 3) % 4, (v + 2) % 4
        low, high = pl.ds(0, WIDE // 2), pl.ds(WIDE // 2, WIDE // 2)
        send(summed.at[g, opposite, :, low], far2.at[g, 0], send2.at[g], recv_far2.at[g], second[0])
        send(summed.at[g, opposite, :, high], far2.at[g, 1], send2.at[g], recv_far2.at[g], second[1])
        send(summed.at[g, up, :, high], near2.at[g, 0, :, high], send2.at[g], recv_near2.at[g], second[0])
        send(summed.at[g, down, :, low], near2.at[g, 1, :, low], send2.at[g], recv_near2.at[g], second[1])

    def relay2(g):
        c, p, h = order[g]
        u, v, first, second = axes(h)
        up, down = (v + 1) % 4, (v + 3) % 4
        low, high = pl.ds(0, WIDE // 2), pl.ds(WIDE // 2, WIDE // 2)
        fake(far2.at[g], far2.at[g], send2.at[g], recv_far2.at[g]).wait_recv()
        summed[g, up, :, low] = (
            summed[g, up, :, low].astype(jnp.float32) + far2[g, 0].astype(jnp.float32)
        ).astype(jnp.bfloat16)
        summed[g, down, :, high] = (
            summed[g, down, :, high].astype(jnp.float32) + far2[g, 1].astype(jnp.float32)
        ).astype(jnp.bfloat16)
        send(summed.at[g, up, :, low], near2.at[g, 0, :, low], send2.at[g], recv_near2.at[g], second[0])
        send(summed.at[g, down, :, high], near2.at[g, 1, :, high], send2.at[g], recv_near2.at[g], second[1])

    def out_copy(g):
        c, p, h = order[g]
        at = (h * PIECES + p) * WIDE
        return pltpu.make_async_copy(
            result.at[g],
            o_hbm.at[pl.ds(c * ROWS, ROWS), pl.ds(at, WIDE)],
            out_sem.at[g],
        )

    def finish(g):
        c, p, h = order[g]
        u, v, first, second = axes(h)
        fake(near2.at[g], near2.at[g], send2.at[g], recv_near2.at[g]).wait_recv()
        result[g] = (
            summed[g, v].astype(jnp.float32)
            + near2[g, 0].astype(jnp.float32)
            + near2[g, 1].astype(jnp.float32)
        ).astype(jnp.bfloat16)
        out_copy(g).start()

    table_load.wait()
    loads[0].wait()
    rotate(0)
    pl.semaphore_wait(barrier, len(OFFSETS))
    exchange(0, mixed, gathered, send_a, recv_a)
    loads[1].wait()
    rotate(1)
    exchange(1, mixed, gathered, send_a, recv_a)
    for load in w_loads:
        load.start()
    for c in range(CHUNKS):
        exchange_all(c, mixed, gathered, send_a, recv_a).wait_recv()
        transform(c)
        exchange(c, quant, dequant, send_q, recv_q)
    each = PIECES * 2
    exchange_all(0, quant, dequant, send_q, recv_q).wait_recv()
    for g in range(each):
        project(g)
    exchange_all(1, quant, dequant, send_q, recv_q).wait_recv()
    for g in range(each):
        project(each + g)
        relay(g)
    for g in range(each):
        relay(each + g)
        gather(g)
    for g in range(each):
        relay2(g)
        gather(each + g)
        finish(g)
    for g in range(each):
        relay2(each + g)
    for g in range(each):
        finish(each + g)

    for c in range(CHUNKS):
        exchange_all(c, mixed, gathered, send_a, recv_a).wait_send()
        exchange_all(c, quant, dequant, send_q, recv_q).wait_send()
    for g in range(2 * each):
        fake(part.at[g, pl.ds(0, 3)], part.at[g, pl.ds(0, 3)], send1.at[g], recv_far.at[g]).wait_send()
        fake(summed.at[g, pl.ds(0, 3)], summed.at[g, pl.ds(0, 3)], send2.at[g], recv_far2.at[g]).wait_send()
        out_copy(g).wait()


def shards(activations, down_weight):
    count_rows, width = activations.shape
    features = down_weight.shape[1]
    table = jnp.asarray(np.kron(sylvester(32), paley_matrix()), jnp.bfloat16)
    bf16, f32 = jnp.bfloat16, jnp.float32
    groups = CHUNKS * PIECES * 2
    dma = pltpu.SemaphoreType.DMA
    any_space = pl.BlockSpec(memory_space=pl.ANY)
    return pl.pallas_call(
        kernel,
        out_shape=jax.ShapeDtypeStruct((count_rows // 16, features), bf16),
        in_specs=[any_space] * 3,
        out_specs=any_space,
        scratch_shapes=[
            pltpu.VMEM((CHUNKS, 16, ROWS, width), bf16),
            pltpu.VMEM(table.shape, bf16),
            pltpu.VMEM((2 * PIECES, width, WIDE), bf16),
            pltpu.VMEM((CHUNKS, 16, ROWS, width), bf16),
            pltpu.VMEM((CHUNKS, 16, ROWS, width), bf16),
            pltpu.VMEM((16, ROWS, width), f32),
            pltpu.VMEM((CHUNKS, 16, ROWS, width), bf16),
            pltpu.VMEM((CHUNKS, 16, ROWS, width), bf16),
            pltpu.VMEM((groups, 4, 4, ROWS, WIDE), bf16),
            pltpu.VMEM((groups, 2, 2, ROWS, WIDE), bf16),
            pltpu.VMEM((groups, 2, 4, ROWS, WIDE), bf16),
            pltpu.VMEM((groups, 4, ROWS, WIDE), bf16),
            pltpu.VMEM((groups, 2, ROWS, WIDE // 2), bf16),
            pltpu.VMEM((groups, 2, ROWS, WIDE), bf16),
            pltpu.VMEM((groups, ROWS, WIDE), bf16),
            dma((CHUNKS + 1,)),
            dma((2 * PIECES,)),
            dma((CHUNKS,)), dma((CHUNKS,)), dma((CHUNKS,)), dma((CHUNKS,)),
            dma((groups,)), dma((groups,)),
            dma((groups,)), dma((groups,)), dma((groups,)), dma((groups,)),
            dma((groups,)),
        ],
        compiler_params=pltpu.CompilerParams(
            collective_id=0, has_side_effects=True, vmem_limit_bytes=62 * 2**20
        ),
        name="rotate_quantize_project",
    )(activations.reshape(16, count_rows // 16, width), table, down_weight)


def solution(mesh):
    placed = (P("dp", "tensor"), P("tensor", None))
    return jax.shard_map(
        shards, mesh=mesh, in_specs=placed, out_specs=P(("dp", "tensor"), None), check_vma=False
    )
```

```python
import functools
import math

import jax
import jax.numpy as jnp
import numpy as np
from jax import lax
from jax.experimental import pallas as pl
from jax.experimental.pallas import tpu as pltpu
from jax.sharding import PartitionSpec as P

MESH = pl.DeviceIdType.MESH
CHUNKS = 2
ROWS = 16
PIECES = 3
WIDE = 1024
TILE = 256
OFFSETS = (
    (0, 1), (1, 0), (0, 3), (3, 0), (1, 1), (3, 3), (1, 3), (3, 1),
    (0, 2), (2, 0), (1, 2), (2, 1), (3, 2), (2, 3), (2, 2),
)


def paley_matrix():
    modulus = 13
    residues = set((value * value % modulus for value in range(1, modulus)))
    confer = np.zeros((14, 14))
    confer[0, 1:] = 1.0
    confer[1:, 0] = 1.0
    for row in range(modulus):
        for col in range(modulus):
            if row != col:
                confer[1 + row, 1 + col] = 1.0 if (col - row) % modulus in residues else -1.0
    return np.kron(confer, np.array([[1.0, 1.0], [1.0, -1.0]])) + np.kron(
        np.eye(14), np.array([[1.0, -1.0], [-1.0, -1.0]])
    )


def sylvester(order):
    matrix = np.ones((1, 1))
    while matrix.shape[0] < order:
        matrix = np.kron(matrix, np.array([[1.0, 1.0], [1.0, -1.0]]))
    return matrix


def sine_coefficients():
    nodes = np.cos(np.pi * (np.arange(64) + 0.5) / 64)
    r2 = 0.125 + 0.125 * nodes
    root = np.sqrt(r2)
    target = np.sinc(2 * root)
    return np.polynomial.chebyshev.Chebyshev.fit(r2, target, 6, domain=[0, 0.25]).convert(
        kind=np.polynomial.Polynomial
    ).coef


SINE = [float(c) for c in sine_coefficients()]


def kernel(
    a_hbm, r_hbm, w_hbm, o_hbm,
    a_in, table, weight, mixed, gathered, rotated, quant, dequant,
    part, far, near, summed, far2, near2, result,
    in_sem, w_sem, send_a, recv_a, send_q, recv_q,
    send1, send2, recv_far, recv_near, recv_far2, recv_near2, out_sem,
):
    me = lax.axis_index("tensor")
    z, y = me // 4, me % 4
    width = a_hbm.shape[-1]
    half = width // 2
    norm = 1.0 / math.sqrt(width * 16)

    def partner(offset):
        return ((z + offset[0]) % 4) * 4 + (y + offset[1]) % 4

    loads = [
        pltpu.make_async_copy(a_hbm.at[:, pl.ds(ROWS * c, ROWS)], a_in.at[c], in_sem.at[c])
        for c in range(CHUNKS)
    ]
    table_load = pltpu.make_async_copy(r_hbm, table, in_sem.at[CHUNKS])
    loads[0].start()
    table_load.start()
    for c in range(1, CHUNKS):
        loads[c].start()
    w_loads = [
        pltpu.make_async_copy(w_hbm.at[:, pl.ds(WIDE * i, WIDE)], weight.at[i], w_sem.at[i])
        for i in range(2 * PIECES)
    ]

    barrier = pltpu.get_barrier_semaphore()
    for offset in OFFSETS:
        pl.semaphore_signal(
            barrier, inc=1, device_id={"tensor": partner(offset)}, device_id_type=MESH
        )

    def rotate(c):
        left = a_in[c, :, :, 0:half].reshape(16 * ROWS, half)
        right = a_in[c, :, :, half:width].reshape(16 * ROWS, half)
        for at in range(0, half, TILE):
            size = min(TILE, half - at)
            cols = table[:, at : at + size]
            first = jnp.dot(left, cols, preferred_element_type=jnp.float32)
            second = jnp.dot(right, cols, preferred_element_type=jnp.float32)
            mixed[c, :, :, at : at + size] = (
                (first + second).astype(jnp.bfloat16).reshape(16, ROWS, size)
            )
            mixed[c, :, :, half + at : half + at + size] = (
                (first - second).astype(jnp.bfloat16).reshape(16, ROWS, size)
            )

    def exchange(c, source, target, send, recv):
        for offset in OFFSETS:
            e = partner(offset)
            pltpu.make_async_remote_copy(
                src_ref=source.at[c, e],
                dst_ref=target.at[c, me],
                send_sem=send.at[c],
                recv_sem=recv.at[c],
                device_id={"tensor": e},
                device_id_type=MESH,
            ).start()
        target[c, me] = source[c, me]

    def exchange_all(c, source, target, send, recv):
        return pltpu.make_async_remote_copy(
            src_ref=source.at[c, pl.ds(0, 15)],
            dst_ref=target.at[c, pl.ds(0, 15)],
            send_sem=send.at[c],
            recv_sem=recv.at[c],
            device_id={"tensor": partner((0, 1))},
            device_id_type=MESH,
        )

    def transform(c):
        def butterfly(t, largest):
            cols = pl.ds(pl.multiple_of(t * 128, 128), 128)
            v = [gathered[c, e, :, cols].astype(jnp.float32) for e in range(16)]
            for bit in (1, 2, 4, 8):
                n = list(v)
                for e in range(16):
                    n[e] = v[e ^ bit] - v[e] if e & bit else v[e] + v[e ^ bit]
                v = n
            for e in range(16):
                rotated[e, :, cols] = v[e]
            m = [jnp.abs(x) for x in v]
            while len(m) > 1:
                m = [jnp.maximum(m[i], m[i + 1]) for i in range(0, len(m), 2)]
            return jnp.maximum(largest, m[0])

        largest = lax.fori_loop(
            0, width // 128, butterfly, jnp.zeros((ROWS, 128), jnp.float32)
        )
        scale = jnp.maximum(jnp.max(largest, axis=1, keepdims=True) * norm, 1.0)
        up = jnp.broadcast_to(7.0 * norm / scale, (ROWS, 128))
        down = jnp.broadcast_to(scale / 7.0, (ROWS, 128))

        def staircase(t, carry):
            cols = pl.ds(pl.multiple_of(t * 128, 128), 128)
            for e in range(16):
                levels = rotated[e, :, cols] * up
                r = levels - jnp.round(levels)
                r2 = r * r
                series = jnp.full_like(r2, SINE[-1])
                for coefficient in SINE[-2::-1]:
                    series = series * r2 + coefficient
                quant[c, e, :, cols] = ((levels - r * series) * down).astype(jnp.bfloat16)
            return carry

        lax.fori_loop(0, width // 128, staircase, 0)

    def axes(h):
        along_y = [partner((0, 1)), partner((0, 3))]
        along_z = [partner((1, 0)), partner((3, 0))]
        return (y, z, along_y, along_z) if h == 0 else (z, y, along_z, along_y)

    def send(source, target, s, r, e):
        pltpu.make_async_remote_copy(
            src_ref=source, dst_ref=target, send_sem=s, recv_sem=r,
            device_id={"tensor": e}, device_id_type=MESH,
        ).start()

    order = [(c, p, h) for c in range(CHUNKS) for p in range(PIECES) for h in range(2)]

    def project(k):
        for g in (2 * k, 2 * k + 1):
            multiply(g)
        flows = [[], []]
        for h in range(2):
            g = 2 * k + h
            u, v, first, second = axes(h)
            up, down, opposite = (u + 1) % 4, (u + 3) % 4, (u + 2) % 4
            flows[h] = [
                (part.at[g, opposite, low], far.at[g, 0], send1.at[g], recv_far.at[g], first[0]),
                (part.at[g, opposite, high], far.at[g, 1], send1.at[g], recv_far.at[g], first[1]),
                (part.at[g, up, high], near.at[g, 0, high], send1.at[g], recv_near.at[g], first[0]),
                (part.at[g, down, low], near.at[g, 1, low], send1.at[g], recv_near.at[g], first[1]),
            ]
        interleave(flows)

    def interleave(flows):
        for pair in zip(*flows):
            for flow in pair:
                send(*flow)

    def multiply(g):
        c, p, h = order[g]
        i = h * PIECES + p
        if c == 0:
            w_loads[i].wait()

        def tile(n, carry):
            cols = pl.ds(pl.multiple_of(n * TILE, TILE), TILE)
            product = jnp.dot(
                dequant[c].reshape(16 * ROWS, width),
                weight[i, :, cols],
                preferred_element_type=jnp.float32,
            ).astype(jnp.bfloat16)
            for e in range(16):
                u, v = (e % 4, e // 4) if h == 0 else (e // 4, e % 4)
                part[g, u, v, :, cols] = product[e * ROWS : (e + 1) * ROWS]
            return carry

        lax.fori_loop(0, WIDE // TILE, tile, 0)

    def fake(source, target, s, r):
        return pltpu.make_async_remote_copy(
            src_ref=source, dst_ref=target, send_sem=s, recv_sem=r,
            device_id={"tensor": partner((0, 1))}, device_id_type=MESH,
        )

    low, high = pl.ds(0, 2), pl.ds(2, 2)
    left, right = pl.ds(0, WIDE // 2), pl.ds(WIDE // 2, WIDE // 2)

    def relay(k):
        flows = [[], []]
        for h in range(2):
            g = 2 * k + h
            u, v, first, second = axes(h)
            up, down = (u + 1) % 4, (u + 3) % 4
            fake(far.at[g], far.at[g], send1.at[g], recv_far.at[g]).wait_recv()
            for j in range(2):
                part[g, up, j] = (
                    part[g, up, j].astype(jnp.float32) + far[g, 0, j].astype(jnp.float32)
                ).astype(jnp.bfloat16)
                part[g, down, 2 + j] = (
                    part[g, down, 2 + j].astype(jnp.float32) + far[g, 1, j].astype(jnp.float32)
                ).astype(jnp.bfloat16)
            flows[h] = [
                (part.at[g, up, low], near.at[g, 0, low], send1.at[g], recv_near.at[g], first[0]),
                (part.at[g, down, high], near.at[g, 1, high], send1.at[g], recv_near.at[g], first[1]),
            ]
        interleave(flows)

    def gather(k):
        flows = [[], []]
        for h in range(2):
            g = 2 * k + h
            u, v, first, second = axes(h)
            fake(near.at[g], near.at[g], send1.at[g], recv_near.at[g]).wait_recv()
            for j in range(4):
                summed[g, j] = (
                    part[g, u, j].astype(jnp.float32)
                    + near[g, 0, j].astype(jnp.float32)
                    + near[g, 1, j].astype(jnp.float32)
                ).astype(jnp.bfloat16)
            up, down, opposite = (v + 1) % 4, (v + 3) % 4, (v + 2) % 4
            flows[h] = [
                (summed.at[g, opposite, :, left], far2.at[g, 0], send2.at[g], recv_far2.at[g], second[0]),
                (summed.at[g, opposite, :, right], far2.at[g, 1], send2.at[g], recv_far2.at[g], second[1]),
                (summed.at[g, up, :, right], near2.at[g, 0, :, right], send2.at[g], recv_near2.at[g], second[0]),
                (summed.at[g, down, :, left], near2.at[g, 1, :, left], send2.at[g], recv_near2.at[g], second[1]),
            ]
        interleave(flows)

    def relay2(k):
        flows = [[], []]
        for h in range(2):
            g = 2 * k + h
            u, v, first, second = axes(h)
            up, down = (v + 1) % 4, (v + 3) % 4
            fake(far2.at[g], far2.at[g], send2.at[g], recv_far2.at[g]).wait_recv()
            summed[g, up, :, left] = (
                summed[g, up, :, left].astype(jnp.float32) + far2[g, 0].astype(jnp.float32)
            ).astype(jnp.bfloat16)
            summed[g, down, :, right] = (
                summed[g, down, :, right].astype(jnp.float32) + far2[g, 1].astype(jnp.float32)
            ).astype(jnp.bfloat16)
            flows[h] = [
                (summed.at[g, up, :, left], near2.at[g, 0, :, left], send2.at[g], recv_near2.at[g], second[0]),
                (summed.at[g, down, :, right], near2.at[g, 1, :, right], send2.at[g], recv_near2.at[g], second[1]),
            ]
        interleave(flows)

    def out_copy(g):
        c, p, h = order[g]
        at = (h * PIECES + p) * WIDE
        return pltpu.make_async_copy(
            result.at[g],
            o_hbm.at[pl.ds(c * ROWS, ROWS), pl.ds(at, WIDE)],
            out_sem.at[g],
        )

    def finish(k):
        for h in range(2):
            g = 2 * k + h
            u, v, first, second = axes(h)
            fake(near2.at[g], near2.at[g], send2.at[g], recv_near2.at[g]).wait_recv()
            result[g] = (
                summed[g, v].astype(jnp.float32)
                + near2[g, 0].astype(jnp.float32)
                + near2[g, 1].astype(jnp.float32)
            ).astype(jnp.bfloat16)
            out_copy(g).start()

    table_load.wait()
    loads[0].wait()
    rotate(0)
    pl.semaphore_wait(barrier, len(OFFSETS))
    exchange(0, mixed, gathered, send_a, recv_a)
    loads[1].wait()
    rotate(1)
    exchange(1, mixed, gathered, send_a, recv_a)
    for load in w_loads:
        load.start()
    for c in range(CHUNKS):
        exchange_all(c, mixed, gathered, send_a, recv_a).wait_recv()
        transform(c)
        exchange(c, quant, dequant, send_q, recv_q)
    each = PIECES
    exchange_all(0, quant, dequant, send_q, recv_q).wait_recv()
    for g in range(each):
        project(g)
    exchange_all(1, quant, dequant, send_q, recv_q).wait_recv()
    for g in range(each):
        project(each + g)
        relay(g)
    for g in range(each):
        relay(each + g)
        gather(g)
    for g in range(each):
        relay2(g)
        gather(each + g)
        finish(g)
    for g in range(each):
        relay2(each + g)
    for g in range(each):
        finish(each + g)

    for c in range(CHUNKS):
        exchange_all(c, mixed, gathered, send_a, recv_a).wait_send()
        exchange_all(c, quant, dequant, send_q, recv_q).wait_send()
    for g in range(len(order)):
        fake(part.at[g, pl.ds(0, 3)], part.at[g, pl.ds(0, 3)], send1.at[g], recv_far.at[g]).wait_send()
        fake(summed.at[g, pl.ds(0, 3)], summed.at[g, pl.ds(0, 3)], send2.at[g], recv_far2.at[g]).wait_send()
        out_copy(g).wait()


def shards(activations, down_weight):
    count_rows, width = activations.shape
    features = down_weight.shape[1]
    table = jnp.asarray(np.kron(sylvester(32), paley_matrix()), jnp.bfloat16)
    bf16, f32 = jnp.bfloat16, jnp.float32
    groups = CHUNKS * PIECES * 2
    dma = pltpu.SemaphoreType.DMA
    any_space = pl.BlockSpec(memory_space=pl.ANY)
    return pl.pallas_call(
        kernel,
        out_shape=jax.ShapeDtypeStruct((count_rows // 16, features), bf16),
        in_specs=[any_space] * 3,
        out_specs=any_space,
        scratch_shapes=[
            pltpu.VMEM((CHUNKS, 16, ROWS, width), bf16),
            pltpu.VMEM(table.shape, bf16),
            pltpu.VMEM((2 * PIECES, width, WIDE), bf16),
            pltpu.VMEM((CHUNKS, 16, ROWS, width), bf16),
            pltpu.VMEM((CHUNKS, 16, ROWS, width), bf16),
            pltpu.VMEM((16, ROWS, width), f32),
            pltpu.VMEM((CHUNKS, 16, ROWS, width), bf16),
            pltpu.VMEM((CHUNKS, 16, ROWS, width), bf16),
            pltpu.VMEM((groups, 4, 4, ROWS, WIDE), bf16),
            pltpu.VMEM((groups, 2, 2, ROWS, WIDE), bf16),
            pltpu.VMEM((groups, 2, 4, ROWS, WIDE), bf16),
            pltpu.VMEM((groups, 4, ROWS, WIDE), bf16),
            pltpu.VMEM((groups, 2, ROWS, WIDE // 2), bf16),
            pltpu.VMEM((groups, 2, ROWS, WIDE), bf16),
            pltpu.VMEM((groups, ROWS, WIDE), bf16),
            dma((CHUNKS + 1,)),
            dma((2 * PIECES,)),
            dma((CHUNKS,)), dma((CHUNKS,)), dma((CHUNKS,)), dma((CHUNKS,)),
            dma((groups,)), dma((groups,)),
            dma((groups,)), dma((groups,)), dma((groups,)), dma((groups,)),
            dma((groups,)),
        ],
        compiler_params=pltpu.CompilerParams(
            collective_id=0, has_side_effects=True, vmem_limit_bytes=62 * 2**20
        ),
        name="rotate_quantize_project",
    )(activations.reshape(16, count_rows // 16, width), table, down_weight)


def solution(mesh):
    placed = (P("dp", "tensor"), P("tensor", None))
    return jax.shard_map(
        shards, mesh=mesh, in_specs=placed, out_specs=P(("dp", "tensor"), None), check_vma=False
    )
```

```python
import functools
import math

import jax
import jax.numpy as jnp
import numpy as np
from jax import lax
from jax.experimental import pallas as pl
from jax.experimental.pallas import tpu as pltpu
from jax.sharding import PartitionSpec as P

MESH = pl.DeviceIdType.MESH
CHUNKS = 2
ROWS = 16
PIECES = 3
WIDE = 1024
DIRECT = (3, 4, 5)
OFFSETS = (
    ((0, 1), (1, 0), (0, 3), (3, 0)),
    ((1, 1), (3, 3), (1, 3), (3, 1), (0, 2), (2, 0)),
    ((1, 2), (2, 1), (3, 2), (2, 3)),
    ((2, 2),),
)


def paley_matrix():
    modulus = 13
    residues = set((value * value % modulus for value in range(1, modulus)))
    confer = np.zeros((14, 14))
    confer[0, 1:] = 1.0
    confer[1:, 0] = 1.0
    for row in range(modulus):
        for col in range(modulus):
            if row != col:
                confer[1 + row, 1 + col] = 1.0 if (col - row) % modulus in residues else -1.0
    return np.kron(confer, np.array([[1.0, 1.0], [1.0, -1.0]])) + np.kron(
        np.eye(14), np.array([[1.0, -1.0], [-1.0, -1.0]])
    )


def sylvester(order):
    matrix = np.ones((1, 1))
    while matrix.shape[0] < order:
        matrix = np.kron(matrix, np.array([[1.0, 1.0], [1.0, -1.0]]))
    return matrix


def sine_coefficients():
    nodes = np.cos(np.pi * (np.arange(64) + 0.5) / 64)
    r2 = 0.125 + 0.125 * nodes
    root = np.sqrt(r2)
    target = np.sinc(2 * root)
    return np.polynomial.chebyshev.Chebyshev.fit(r2, target, 6, domain=[0, 0.25]).convert(
        kind=np.polynomial.Polynomial
    ).coef


SINE = [float(c) for c in sine_coefficients()]


def kernel(
    a_hbm, r_hbm, w_hbm, o_hbm,
    a_in, table, weight, mixed, gathered, rotated, quant, dequant,
    part, far, near, summed, far2, near2, result,
    in_sem, w_sem, send_a, recv_a, send_q, recv_q,
    send1, send2, recv_far, recv_near, recv_far2, recv_near2, out_sem, heard,
):
    me = lax.axis_index("tensor")
    z, y = me // 4, me % 4
    width = a_hbm.shape[-1]
    half = width // 2
    norm = 1.0 / math.sqrt(width * 16)

    def partner(offset):
        return ((z + offset[0]) % 4) * 4 + (y + offset[1]) % 4

    loads = [
        pltpu.make_async_copy(a_hbm.at[:, pl.ds(ROWS * c, ROWS)], a_in.at[c], in_sem.at[c])
        for c in range(CHUNKS)
    ]
    table_load = pltpu.make_async_copy(r_hbm, table, in_sem.at[CHUNKS])
    loads[0].start()
    table_load.start()
    for c in range(1, CHUNKS):
        loads[c].start()
    w_loads = [
        pltpu.make_async_copy(w_hbm.at[:, pl.ds(WIDE * i, WIDE)], weight.at[i], w_sem.at[i])
        for i in range(2 * PIECES)
    ]

    barrier = pltpu.get_barrier_semaphore()
    for offset in OFFSETS[0]:
        pl.semaphore_signal(
            barrier, inc=1, device_id={"tensor": partner(offset)}, device_id_type=MESH
        )

    def hear(stage):
        pl.semaphore_wait(barrier if stage == 0 else heard.at[stage - 1], 4)
        if stage < 3:
            for offset in OFFSETS[0]:
                pl.semaphore_signal(
                    heard.at[stage], inc=1,
                    device_id={"tensor": partner(offset)}, device_id_type=MESH,
                )

    def rotate(c):
        left = a_in[c, :, :, 0:half].reshape(16 * ROWS, half)
        right = a_in[c, :, :, half:width].reshape(16 * ROWS, half)
        for at in range(0, half, 256):
            size = min(256, half - at)
            cols = table[:, at : at + size]
            first = jnp.dot(left, cols, preferred_element_type=jnp.float32)
            second = jnp.dot(right, cols, preferred_element_type=jnp.float32)
            mixed[c, :, :, at : at + size] = (
                (first + second).astype(jnp.bfloat16).reshape(16, ROWS, size)
            )
            mixed[c, :, :, half + at : half + at + size] = (
                (first - second).astype(jnp.bfloat16).reshape(16, ROWS, size)
            )

    def exchange(c, stages, source, target, send, recv):
        for offset in sum((OFFSETS[stage] for stage in stages), ()):
            e = partner(offset)
            pltpu.make_async_remote_copy(
                src_ref=source.at[c, e],
                dst_ref=target.at[c, me],
                send_sem=send.at[c],
                recv_sem=recv.at[c],
                device_id={"tensor": e},
                device_id_type=MESH,
            ).start()

    def exchange_all(c, source, target, send, recv):
        return pltpu.make_async_remote_copy(
            src_ref=source.at[c, pl.ds(0, 15)],
            dst_ref=target.at[c, pl.ds(0, 15)],
            send_sem=send.at[c],
            recv_sem=recv.at[c],
            device_id={"tensor": partner((0, 1))},
            device_id_type=MESH,
        )

    def transform(c):
        def butterfly(t, largest):
            cols = pl.ds(pl.multiple_of(t * 128, 128), 128)
            v = [gathered[c, e, :, cols].astype(jnp.float32) for e in range(16)]
            for bit in (1, 2, 4, 8):
                n = list(v)
                for e in range(16):
                    n[e] = v[e ^ bit] - v[e] if e & bit else v[e] + v[e ^ bit]
                v = n
            for e in range(16):
                rotated[e, :, cols] = v[e]
            m = [jnp.abs(x) for x in v]
            while len(m) > 1:
                m = [jnp.maximum(m[i], m[i + 1]) for i in range(0, len(m), 2)]
            return jnp.maximum(largest, m[0])

        largest = lax.fori_loop(
            0, width // 128, butterfly, jnp.zeros((ROWS, 128), jnp.float32)
        )
        scale = jnp.maximum(jnp.max(largest, axis=1, keepdims=True) * norm, 1.0)
        up = jnp.broadcast_to(7.0 * norm / scale, (ROWS, 128))
        down = jnp.broadcast_to(scale / 7.0, (ROWS, 128))

        def staircase(t, carry):
            cols = pl.ds(pl.multiple_of(t * 128, 128), 128)
            for e in range(16):
                levels = rotated[e, :, cols] * up
                r = levels - jnp.round(levels)
                r2 = r * r
                series = jnp.full_like(r2, SINE[-1])
                for coefficient in SINE[-2::-1]:
                    series = series * r2 + coefficient
                quant[c, e, :, cols] = ((levels - r * series) * down).astype(jnp.bfloat16)
            return carry

        lax.fori_loop(0, width // 128, staircase, 0)

    def axes(h):
        along_y = [partner((0, 1)), partner((0, 3)), partner((0, 2))]
        along_z = [partner((1, 0)), partner((3, 0)), partner((2, 0))]
        return (y, z, along_y, along_z) if h == 0 else (z, y, along_z, along_y)

    def send(source, target, s, r, e):
        pltpu.make_async_remote_copy(
            src_ref=source, dst_ref=target, send_sem=s, recv_sem=r,
            device_id={"tensor": e}, device_id_type=MESH,
        ).start()

    order = [(c, p, h) for c in range(CHUNKS) for p in range(PIECES) for h in range(2)]

    def project(k):
        for g in (2 * k, 2 * k + 1):
            multiply(g)
        flows = [[], []]
        for h in range(2):
            g = 2 * k + h
            u, v, first, second = axes(h)
            up, down, opposite = (u + 1) % 4, (u + 3) % 4, (u + 2) % 4
            flows[h] = [
                (part.at[g, opposite, low], far.at[g, 0], send1.at[g], recv_far.at[g], first[0]),
                (part.at[g, opposite, high], far.at[g, 1], send1.at[g], recv_far.at[g], first[1]),
                (part.at[g, up, high], near.at[g, 0, high], send1.at[g], recv_near.at[g], first[0]),
                (part.at[g, down, low], near.at[g, 1, low], send1.at[g], recv_near.at[g], first[1]),
            ]
        interleave(flows)

    def interleave(flows):
        for pair in zip(*flows):
            for flow in pair:
                send(*flow)

    def multiply(g):
        c, p, h = order[g]
        i = h * PIECES + p
        if c == 0:
            w_loads[i].wait()

        product = jnp.dot(
            dequant[c].reshape(16 * ROWS, width), weight[i], preferred_element_type=jnp.float32
        ).astype(jnp.bfloat16)
        for e in range(16):
            u, v = (e % 4, e // 4) if h == 0 else (e // 4, e % 4)
            part[g, u, v] = product[e * ROWS : (e + 1) * ROWS]

    def fake(source, target, s, r):
        return pltpu.make_async_remote_copy(
            src_ref=source, dst_ref=target, send_sem=s, recv_sem=r,
            device_id={"tensor": partner((0, 1))}, device_id_type=MESH,
        )

    low, high = pl.ds(0, 2), pl.ds(2, 2)
    left, right = pl.ds(0, WIDE // 2), pl.ds(WIDE // 2, WIDE // 2)

    def relay(k):
        flows = [[], []]
        for h in range(2):
            g = 2 * k + h
            u, v, first, second = axes(h)
            up, down = (u + 1) % 4, (u + 3) % 4
            fake(far.at[g], far.at[g], send1.at[g], recv_far.at[g]).wait_recv()
            for j in range(2):
                part[g, up, j] = (
                    part[g, up, j].astype(jnp.float32) + far[g, 0, j].astype(jnp.float32)
                ).astype(jnp.bfloat16)
                part[g, down, 2 + j] = (
                    part[g, down, 2 + j].astype(jnp.float32) + far[g, 1, j].astype(jnp.float32)
                ).astype(jnp.bfloat16)
            flows[h] = [
                (part.at[g, up, low], near.at[g, 0, low], send1.at[g], recv_near.at[g], first[0]),
                (part.at[g, down, high], near.at[g, 1, high], send1.at[g], recv_near.at[g], first[1]),
            ]
        interleave(flows)

    def gather(k):
        flows = [[], []]
        for h in range(2):
            g = 2 * k + h
            u, v, first, second = axes(h)
            fake(near.at[g], near.at[g], send1.at[g], recv_near.at[g]).wait_recv()
            for j in range(4):
                summed[g, j] = (
                    part[g, u, j].astype(jnp.float32)
                    + near[g, 0, j].astype(jnp.float32)
                    + near[g, 1, j].astype(jnp.float32)
                ).astype(jnp.bfloat16)
            up, down, opposite = (v + 1) % 4, (v + 3) % 4, (v + 2) % 4
            if k in DIRECT:
                flows[h] = [
                    (summed.at[g, opposite], near2.at[g, 2], send2.at[g], recv_near2.at[g], second[2]),
                    (summed.at[g, up], near2.at[g, 0], send2.at[g], recv_near2.at[g], second[0]),
                    (summed.at[g, down], near2.at[g, 1], send2.at[g], recv_near2.at[g], second[1]),
                ]
                continue
            flows[h] = [
                (summed.at[g, opposite, :, left], far2.at[g, 0], send2.at[g], recv_far2.at[g], second[0]),
                (summed.at[g, opposite, :, right], far2.at[g, 1], send2.at[g], recv_far2.at[g], second[1]),
                (summed.at[g, up, :, right], near2.at[g, 0, :, right], send2.at[g], recv_near2.at[g], second[0]),
                (summed.at[g, down, :, left], near2.at[g, 1, :, left], send2.at[g], recv_near2.at[g], second[1]),
            ]
        interleave(flows)

    def relay2(k):
        if k in DIRECT:
            return
        flows = [[], []]
        for h in range(2):
            g = 2 * k + h
            u, v, first, second = axes(h)
            up, down = (v + 1) % 4, (v + 3) % 4
            fake(far2.at[g], far2.at[g], send2.at[g], recv_far2.at[g]).wait_recv()
            summed[g, up, :, left] = (
                summed[g, up, :, left].astype(jnp.float32) + far2[g, 0].astype(jnp.float32)
            ).astype(jnp.bfloat16)
            summed[g, down, :, right] = (
                summed[g, down, :, right].astype(jnp.float32) + far2[g, 1].astype(jnp.float32)
            ).astype(jnp.bfloat16)
            flows[h] = [
                (summed.at[g, up, :, left], near2.at[g, 0, :, left], send2.at[g], recv_near2.at[g], second[0]),
                (summed.at[g, down, :, right], near2.at[g, 1, :, right], send2.at[g], recv_near2.at[g], second[1]),
            ]
        interleave(flows)

    def out_copy(g):
        c, p, h = order[g]
        at = (h * PIECES + p) * WIDE
        return pltpu.make_async_copy(
            result.at[g],
            o_hbm.at[pl.ds(c * ROWS, ROWS), pl.ds(at, WIDE)],
            out_sem.at[g],
        )

    def finish(k):
        for h in range(2):
            g = 2 * k + h
            u, v, first, second = axes(h)
            count = 3 if k in DIRECT else 2
            landed = near2.at[g, pl.ds(0, count)]
            fake(landed, landed, send2.at[g], recv_near2.at[g]).wait_recv()
            total = summed[g, v].astype(jnp.float32)
            for j in range(count):
                total = total + near2[g, j].astype(jnp.float32)
            result[g] = total.astype(jnp.bfloat16)
            out_copy(g).start()

    hear(0)
    table_load.wait()
    loads[0].wait()
    rotate(0)
    for stage in range(4):
        if stage > 0:
            hear(stage)
        exchange(0, (stage,), mixed, gathered, send_a, recv_a)
        if stage == 1:
            loads[1].wait()
            rotate(1)
    exchange(1, range(4), mixed, gathered, send_a, recv_a)
    for load in w_loads:
        load.start()
    for c in range(CHUNKS):
        gathered[c, me] = mixed[c, me]
        exchange_all(c, mixed, gathered, send_a, recv_a).wait_recv()
        transform(c)
        exchange(c, range(4), quant, dequant, send_q, recv_q)
        dequant[c, me] = quant[c, me]
    each = PIECES
    exchange_all(0, quant, dequant, send_q, recv_q).wait_recv()
    for g in range(each):
        project(g)
    exchange_all(1, quant, dequant, send_q, recv_q).wait_recv()
    for g in range(each):
        project(each + g)
        relay(g)
    for g in range(each):
        relay(each + g)
        gather(g)
    for g in range(each):
        relay2(g)
        gather(each + g)
    for g in range(each):
        finish(g)
        relay2(each + g)
    for g in range(each):
        finish(each + g)

    for c in range(CHUNKS):
        exchange_all(c, mixed, gathered, send_a, recv_a).wait_send()
        exchange_all(c, quant, dequant, send_q, recv_q).wait_send()
    for g in range(len(order)):
        fake(part.at[g, pl.ds(0, 3)], part.at[g, pl.ds(0, 3)], send1.at[g], recv_far.at[g]).wait_send()
        fake(summed.at[g, pl.ds(0, 3)], summed.at[g, pl.ds(0, 3)], send2.at[g], recv_far2.at[g]).wait_send()
        out_copy(g).wait()


def shards(activations, down_weight):
    count_rows, width = activations.shape
    features = down_weight.shape[1]
    table = jnp.asarray(np.kron(sylvester(32), paley_matrix()), jnp.bfloat16)
    bf16, f32 = jnp.bfloat16, jnp.float32
    groups = CHUNKS * PIECES * 2
    dma = pltpu.SemaphoreType.DMA
    any_space = pl.BlockSpec(memory_space=pl.ANY)
    return pl.pallas_call(
        kernel,
        out_shape=jax.ShapeDtypeStruct((count_rows // 16, features), bf16),
        in_specs=[any_space] * 3,
        out_specs=any_space,
        scratch_shapes=[
            pltpu.VMEM((CHUNKS, 16, ROWS, width), bf16),
            pltpu.VMEM(table.shape, bf16),
            pltpu.VMEM((2 * PIECES, width, WIDE), bf16),
            pltpu.VMEM((CHUNKS, 16, ROWS, width), bf16),
            pltpu.VMEM((CHUNKS, 16, ROWS, width), bf16),
            pltpu.VMEM((16, ROWS, width), f32),
            pltpu.VMEM((CHUNKS, 16, ROWS, width), bf16),
            pltpu.VMEM((CHUNKS, 16, ROWS, width), bf16),
            pltpu.VMEM((groups, 4, 4, ROWS, WIDE), bf16),
            pltpu.VMEM((groups, 2, 2, ROWS, WIDE), bf16),
            pltpu.VMEM((groups, 2, 4, ROWS, WIDE), bf16),
            pltpu.VMEM((groups, 4, ROWS, WIDE), bf16),
            pltpu.VMEM((groups, 2, ROWS, WIDE // 2), bf16),
            pltpu.VMEM((groups, 3, ROWS, WIDE), bf16),
            pltpu.VMEM((groups, ROWS, WIDE), bf16),
            dma((CHUNKS + 1,)),
            dma((2 * PIECES,)),
            dma((CHUNKS,)), dma((CHUNKS,)), dma((CHUNKS,)), dma((CHUNKS,)),
            dma((groups,)), dma((groups,)),
            dma((groups,)), dma((groups,)), dma((groups,)), dma((groups,)),
            dma((groups,)),
            pltpu.SemaphoreType.REGULAR((3,)),
        ],
        compiler_params=pltpu.CompilerParams(
            collective_id=0, has_side_effects=True, vmem_limit_bytes=62 * 2**20
        ),
        name="rotate_quantize_project",
    )(activations.reshape(16, count_rows // 16, width), table, down_weight)


def solution(mesh):
    placed = (P("dp", "tensor"), P("tensor", None))
    return jax.shard_map(
        shards, mesh=mesh, in_specs=placed, out_specs=P(("dp", "tensor"), None), check_vma=False
    )
```

```python
import functools
import math

import jax
import jax.numpy as jnp
import numpy as np
from jax import lax
from jax.experimental import pallas as pl
from jax.experimental.pallas import tpu as pltpu
from jax.sharding import PartitionSpec as P

MESH = pl.DeviceIdType.MESH
CHUNKS = 2
ROWS = 16
PIECES = 3
WIDE = 1024
DIRECT = (3, 4, 5)
OFFSETS = (
    ((0, 1), (1, 0), (0, 3), (3, 0)),
    ((1, 1), (3, 3), (1, 3), (3, 1), (0, 2), (2, 0)),
    ((1, 2), (2, 1), (3, 2), (2, 3)),
    ((2, 2),),
)


def paley_matrix():
    modulus = 13
    residues = set((value * value % modulus for value in range(1, modulus)))
    confer = np.zeros((14, 14))
    confer[0, 1:] = 1.0
    confer[1:, 0] = 1.0
    for row in range(modulus):
        for col in range(modulus):
            if row != col:
                confer[1 + row, 1 + col] = 1.0 if (col - row) % modulus in residues else -1.0
    return np.kron(confer, np.array([[1.0, 1.0], [1.0, -1.0]])) + np.kron(
        np.eye(14), np.array([[1.0, -1.0], [-1.0, -1.0]])
    )


def sylvester(order):
    matrix = np.ones((1, 1))
    while matrix.shape[0] < order:
        matrix = np.kron(matrix, np.array([[1.0, 1.0], [1.0, -1.0]]))
    return matrix


def sine_coefficients():
    nodes = np.cos(np.pi * (np.arange(64) + 0.5) / 64)
    r2 = 0.125 + 0.125 * nodes
    root = np.sqrt(r2)
    target = np.sinc(2 * root)
    return np.polynomial.chebyshev.Chebyshev.fit(r2, target, 6, domain=[0, 0.25]).convert(
        kind=np.polynomial.Polynomial
    ).coef


SINE = [float(c) for c in sine_coefficients()]


def kernel(
    a_hbm, r_hbm, w_hbm, out,
    a_in, table, weight, mixed, gathered, rotated, quant, dequant,
    part, far, near, summed, far2, near2,
    in_sem, w_sem, send_a, recv_a, send_q, recv_q,
    send1, send2, recv_far, recv_near, recv_far2, recv_near2, heard,
):
    me = lax.axis_index("tensor")
    z, y = me // 4, me % 4
    width = a_hbm.shape[-1]
    half = width // 2
    norm = 1.0 / math.sqrt(width * 16)

    def partner(offset):
        return ((z + offset[0]) % 4) * 4 + (y + offset[1]) % 4

    loads = [
        pltpu.make_async_copy(a_hbm.at[:, pl.ds(ROWS * c, ROWS)], a_in.at[c], in_sem.at[c])
        for c in range(CHUNKS)
    ]
    table_load = pltpu.make_async_copy(r_hbm, table, in_sem.at[CHUNKS])
    loads[0].start()
    table_load.start()
    for c in range(1, CHUNKS):
        loads[c].start()
    w_loads = [
        pltpu.make_async_copy(w_hbm.at[:, pl.ds(WIDE * i, WIDE)], weight.at[i], w_sem.at[i])
        for i in range(2 * PIECES)
    ]

    barrier = pltpu.get_barrier_semaphore()
    for offset in OFFSETS[0]:
        pl.semaphore_signal(
            barrier, inc=1, device_id={"tensor": partner(offset)}, device_id_type=MESH
        )

    def hear(stage):
        pl.semaphore_wait(barrier if stage == 0 else heard.at[stage - 1], 4)
        if stage < 3:
            for offset in OFFSETS[0]:
                pl.semaphore_signal(
                    heard.at[stage], inc=1,
                    device_id={"tensor": partner(offset)}, device_id_type=MESH,
                )

    def rotate(c, places):
        rows = [a_in[c, e] for e in places]
        left = jnp.concatenate([row[:, 0:half] for row in rows], axis=0)
        right = jnp.concatenate([row[:, half:width] for row in rows], axis=0)
        for at in range(0, half, 256):
            size = min(256, half - at)
            cols = table[:, at : at + size]
            first = jnp.dot(left, cols, preferred_element_type=jnp.float32)
            second = jnp.dot(right, cols, preferred_element_type=jnp.float32)
            plus, minus = (first + second).astype(jnp.bfloat16), (first - second).astype(jnp.bfloat16)
            for i, e in enumerate(places):
                here = slice(i * ROWS, (i + 1) * ROWS)
                mixed[c, e, :, at : at + size] = plus[here]
                mixed[c, e, :, half + at : half + at + size] = minus[here]

    def exchange(c, stages, source, target, send, recv):
        for offset in sum((OFFSETS[stage] for stage in stages), ()):
            e = partner(offset)
            pltpu.make_async_remote_copy(
                src_ref=source.at[c, e],
                dst_ref=target.at[c, me],
                send_sem=send.at[c],
                recv_sem=recv.at[c],
                device_id={"tensor": e},
                device_id_type=MESH,
            ).start()

    def exchange_all(c, source, target, send, recv):
        return pltpu.make_async_remote_copy(
            src_ref=source.at[c, pl.ds(0, 15)],
            dst_ref=target.at[c, pl.ds(0, 15)],
            send_sem=send.at[c],
            recv_sem=recv.at[c],
            device_id={"tensor": partner((0, 1))},
            device_id_type=MESH,
        )

    def transform(c):
        def butterfly(t, largest):
            cols = pl.ds(pl.multiple_of(t * 128, 128), 128)
            v = [gathered[c, e, :, cols].astype(jnp.float32) for e in range(16)]
            for bit in (1, 2, 4, 8):
                n = list(v)
                for e in range(16):
                    n[e] = v[e ^ bit] - v[e] if e & bit else v[e] + v[e ^ bit]
                v = n
            for e in range(16):
                rotated[e, :, cols] = v[e]
            m = [jnp.abs(x) for x in v]
            while len(m) > 1:
                m = [jnp.maximum(m[i], m[i + 1]) for i in range(0, len(m), 2)]
            return jnp.maximum(largest, m[0])

        largest = lax.fori_loop(
            0, width // 128, butterfly, jnp.zeros((ROWS, 128), jnp.float32)
        )
        scale = jnp.maximum(jnp.max(largest, axis=1, keepdims=True) * norm, 1.0)
        up = jnp.broadcast_to(7.0 * norm / scale, (ROWS, 128))
        down = jnp.broadcast_to(scale / 7.0, (ROWS, 128))

        def staircase(t, carry):
            cols = pl.ds(pl.multiple_of(t * 128, 128), 128)
            for e in range(16):
                levels = rotated[e, :, cols] * up
                r = levels - jnp.round(levels)
                r2 = r * r
                series = jnp.full_like(r2, SINE[-1])
                for coefficient in SINE[-2::-1]:
                    series = series * r2 + coefficient
                quant[c, e, :, cols] = ((levels - r * series) * down).astype(jnp.bfloat16)
            return carry

        lax.fori_loop(0, width // 128, staircase, 0)

    def axes(h):
        along_y = [partner((0, 1)), partner((0, 3)), partner((0, 2))]
        along_z = [partner((1, 0)), partner((3, 0)), partner((2, 0))]
        return (y, z, along_y, along_z) if h == 0 else (z, y, along_z, along_y)

    def send(source, target, s, r, e):
        pltpu.make_async_remote_copy(
            src_ref=source, dst_ref=target, send_sem=s, recv_sem=r,
            device_id={"tensor": e}, device_id_type=MESH,
        ).start()

    order = [(c, p, h) for c in range(CHUNKS) for p in range(PIECES) for h in range(2)]

    def project(k):
        for g in (2 * k, 2 * k + 1):
            multiply(g)
        flows = [[], []]
        for h in range(2):
            g = 2 * k + h
            u, v, first, second = axes(h)
            up, down, opposite = (u + 1) % 4, (u + 3) % 4, (u + 2) % 4
            flows[h] = [
                (part.at[g, opposite, low], far.at[g, 0], send1.at[g], recv_far.at[g], first[0]),
                (part.at[g, opposite, high], far.at[g, 1], send1.at[g], recv_far.at[g], first[1]),
                (part.at[g, up, high], near.at[g, 0, high], send1.at[g], recv_near.at[g], first[0]),
                (part.at[g, down, low], near.at[g, 1, low], send1.at[g], recv_near.at[g], first[1]),
            ]
        interleave(flows)

    def interleave(flows):
        for pair in zip(*flows):
            for flow in pair:
                send(*flow)

    def multiply(g):
        c, p, h = order[g]
        i = h * PIECES + p
        if c == 0:
            w_loads[i].wait()

        product = jnp.dot(
            dequant[c].reshape(16 * ROWS, width), weight[i], preferred_element_type=jnp.float32
        ).astype(jnp.bfloat16)
        for e in range(16):
            u, v = (e % 4, e // 4) if h == 0 else (e // 4, e % 4)
            part[g, u, v] = product[e * ROWS : (e + 1) * ROWS]

    def fake(source, target, s, r):
        return pltpu.make_async_remote_copy(
            src_ref=source, dst_ref=target, send_sem=s, recv_sem=r,
            device_id={"tensor": partner((0, 1))}, device_id_type=MESH,
        )

    low, high = pl.ds(0, 2), pl.ds(2, 2)
    left, right = pl.ds(0, WIDE // 2), pl.ds(WIDE // 2, WIDE // 2)

    def relay(k):
        flows = [[], []]
        for h in range(2):
            g = 2 * k + h
            u, v, first, second = axes(h)
            up, down = (u + 1) % 4, (u + 3) % 4
            fake(far.at[g], far.at[g], send1.at[g], recv_far.at[g]).wait_recv()
            for j in range(2):
                part[g, up, j] = (
                    part[g, up, j].astype(jnp.float32) + far[g, 0, j].astype(jnp.float32)
                ).astype(jnp.bfloat16)
                part[g, down, 2 + j] = (
                    part[g, down, 2 + j].astype(jnp.float32) + far[g, 1, j].astype(jnp.float32)
                ).astype(jnp.bfloat16)
            flows[h] = [
                (part.at[g, up, low], near.at[g, 0, low], send1.at[g], recv_near.at[g], first[0]),
                (part.at[g, down, high], near.at[g, 1, high], send1.at[g], recv_near.at[g], first[1]),
            ]
        interleave(flows)

    def gather(k):
        flows = [[], []]
        for h in range(2):
            g = 2 * k + h
            u, v, first, second = axes(h)
            fake(near.at[g], near.at[g], send1.at[g], recv_near.at[g]).wait_recv()
            for j in range(4):
                summed[g, j] = (
                    part[g, u, j].astype(jnp.float32)
                    + near[g, 0, j].astype(jnp.float32)
                    + near[g, 1, j].astype(jnp.float32)
                ).astype(jnp.bfloat16)
            up, down, opposite = (v + 1) % 4, (v + 3) % 4, (v + 2) % 4
            if k in DIRECT:
                flows[h] = [
                    (summed.at[g, opposite], near2.at[g, 2], send2.at[g], recv_near2.at[g], second[2]),
                    (summed.at[g, up], near2.at[g, 0], send2.at[g], recv_near2.at[g], second[0]),
                    (summed.at[g, down], near2.at[g, 1], send2.at[g], recv_near2.at[g], second[1]),
                ]
                continue
            flows[h] = [
                (summed.at[g, opposite, :, left], far2.at[g, 0], send2.at[g], recv_far2.at[g], second[0]),
                (summed.at[g, opposite, :, right], far2.at[g, 1], send2.at[g], recv_far2.at[g], second[1]),
                (summed.at[g, up, :, right], near2.at[g, 0, :, right], send2.at[g], recv_near2.at[g], second[0]),
                (summed.at[g, down, :, left], near2.at[g, 1, :, left], send2.at[g], recv_near2.at[g], second[1]),
            ]
        interleave(flows)

    def relay2(k):
        if k in DIRECT:
            return
        flows = [[], []]
        for h in range(2):
            g = 2 * k + h
            u, v, first, second = axes(h)
            up, down = (v + 1) % 4, (v + 3) % 4
            fake(far2.at[g], far2.at[g], send2.at[g], recv_far2.at[g]).wait_recv()
            summed[g, up, :, left] = (
                summed[g, up, :, left].astype(jnp.float32) + far2[g, 0].astype(jnp.float32)
            ).astype(jnp.bfloat16)
            summed[g, down, :, right] = (
                summed[g, down, :, right].astype(jnp.float32) + far2[g, 1].astype(jnp.float32)
            ).astype(jnp.bfloat16)
            flows[h] = [
                (summed.at[g, up, :, left], near2.at[g, 0, :, left], send2.at[g], recv_near2.at[g], second[0]),
                (summed.at[g, down, :, right], near2.at[g, 1, :, right], send2.at[g], recv_near2.at[g], second[1]),
            ]
        interleave(flows)

    def finish(k):
        for h in range(2):
            g = 2 * k + h
            c, p, _ = order[g]
            u, v, first, second = axes(h)
            count = 3 if k in DIRECT else 2
            landed = near2.at[g, pl.ds(0, count)]
            fake(landed, landed, send2.at[g], recv_near2.at[g]).wait_recv()
            total = summed[g, v].astype(jnp.float32)
            for j in range(count):
                total = total + near2[g, j].astype(jnp.float32)
            at = (h * PIECES + p) * WIDE
            out[c * ROWS : (c + 1) * ROWS, at : at + WIDE] = total.astype(jnp.bfloat16)

    hear(0)
    table_load.wait()
    loads[0].wait()
    for stage in range(4):
        if stage < 2:
            rotate(0, [partner(o) for o in OFFSETS[stage]])
        if stage == 2:
            rotate(0, [partner(o) for o in OFFSETS[2] + OFFSETS[3]] + [me])
        if stage > 0:
            hear(stage)
        exchange(0, (stage,), mixed, gathered, send_a, recv_a)
    loads[1].wait()
    rotate(1, list(range(16)))
    exchange(1, range(4), mixed, gathered, send_a, recv_a)
    for load in w_loads:
        load.start()
    for c in range(CHUNKS):
        gathered[c, me] = mixed[c, me]
        exchange_all(c, mixed, gathered, send_a, recv_a).wait_recv()
        transform(c)
        exchange(c, range(4), quant, dequant, send_q, recv_q)
        dequant[c, me] = quant[c, me]
    each = PIECES
    exchange_all(0, quant, dequant, send_q, recv_q).wait_recv()
    for g in range(each):
        project(g)
    exchange_all(1, quant, dequant, send_q, recv_q).wait_recv()
    for g in range(each):
        project(each + g)
        relay(g)
    for g in range(each):
        relay(each + g)
        gather(g)
    for g in range(each):
        relay2(g)
        gather(each + g)
    for g in range(each):
        finish(g)
        relay2(each + g)
    for g in range(each):
        finish(each + g)

    for c in range(CHUNKS):
        exchange_all(c, mixed, gathered, send_a, recv_a).wait_send()
        exchange_all(c, quant, dequant, send_q, recv_q).wait_send()
    for g in range(len(order)):
        fake(part.at[g, pl.ds(0, 3)], part.at[g, pl.ds(0, 3)], send1.at[g], recv_far.at[g]).wait_send()
        fake(summed.at[g, pl.ds(0, 3)], summed.at[g, pl.ds(0, 3)], send2.at[g], recv_far2.at[g]).wait_send()


def shards(activations, down_weight):
    count_rows, width = activations.shape
    features = down_weight.shape[1]
    table = jnp.asarray(np.kron(sylvester(32), paley_matrix()), jnp.bfloat16)
    bf16, f32 = jnp.bfloat16, jnp.float32
    groups = CHUNKS * PIECES * 2
    dma = pltpu.SemaphoreType.DMA
    return pl.pallas_call(
        kernel,
        out_shape=jax.ShapeDtypeStruct((count_rows // 16, features), bf16),
        in_specs=[pl.BlockSpec(memory_space=pltpu.HBM)] * 3,
        out_specs=pl.BlockSpec(memory_space=pltpu.VMEM),
        scratch_shapes=[
            pltpu.VMEM((CHUNKS, 16, ROWS, width), bf16),
            pltpu.VMEM(table.shape, bf16),
            pltpu.VMEM((2 * PIECES, width, WIDE), bf16),
            pltpu.VMEM((CHUNKS, 16, ROWS, width), bf16),
            pltpu.VMEM((CHUNKS, 16, ROWS, width), bf16),
            pltpu.VMEM((16, ROWS, width), f32),
            pltpu.VMEM((CHUNKS, 16, ROWS, width), bf16),
            pltpu.VMEM((CHUNKS, 16, ROWS, width), bf16),
            pltpu.VMEM((groups, 4, 4, ROWS, WIDE), bf16),
            pltpu.VMEM((groups, 2, 2, ROWS, WIDE), bf16),
            pltpu.VMEM((groups, 2, 4, ROWS, WIDE), bf16),
            pltpu.VMEM((groups, 4, ROWS, WIDE), bf16),
            pltpu.VMEM((groups, 2, ROWS, WIDE // 2), bf16),
            pltpu.VMEM((groups, 3, ROWS, WIDE), bf16),
            dma((CHUNKS + 1,)),
            dma((2 * PIECES,)),
            dma((CHUNKS,)), dma((CHUNKS,)), dma((CHUNKS,)), dma((CHUNKS,)),
            dma((groups,)), dma((groups,)),
            dma((groups,)), dma((groups,)), dma((groups,)), dma((groups,)),
            pltpu.SemaphoreType.REGULAR((3,)),
        ],
        compiler_params=pltpu.CompilerParams(
            collective_id=0, has_side_effects=True, vmem_limit_bytes=53 * 2**20
        ),
        name="rotate_quantize_project",
    )(activations.reshape(16, count_rows // 16, width), table, down_weight)


def solution(mesh):
    placed = (P("dp", "tensor"), P("tensor", None))
    return jax.shard_map(
        shards, mesh=mesh, in_specs=placed, out_specs=P(("dp", "tensor"), None), check_vma=False
    )
```

```python
import functools
import math

import jax
import jax.numpy as jnp
import numpy as np
from jax import lax
from jax.experimental import pallas as pl
from jax.experimental.pallas import tpu as pltpu
from jax.sharding import PartitionSpec as P

MESH = pl.DeviceIdType.MESH
CHUNKS = 2
ROWS = 16
PIECES = 3
WIDE = 1024
DIRECT = (3, 4, 5)
OFFSETS = (
    ((0, 1), (1, 0), (0, 3), (3, 0)),
    ((1, 1), (3, 3), (1, 3), (3, 1), (0, 2), (2, 0)),
    ((1, 2), (2, 1), (3, 2), (2, 3)),
    ((2, 2),),
)


def paley_matrix():
    modulus = 13
    residues = set((value * value % modulus for value in range(1, modulus)))
    confer = np.zeros((14, 14))
    confer[0, 1:] = 1.0
    confer[1:, 0] = 1.0
    for row in range(modulus):
        for col in range(modulus):
            if row != col:
                confer[1 + row, 1 + col] = 1.0 if (col - row) % modulus in residues else -1.0
    return np.kron(confer, np.array([[1.0, 1.0], [1.0, -1.0]])) + np.kron(
        np.eye(14), np.array([[1.0, -1.0], [-1.0, -1.0]])
    )


def sylvester(order):
    matrix = np.ones((1, 1))
    while matrix.shape[0] < order:
        matrix = np.kron(matrix, np.array([[1.0, 1.0], [1.0, -1.0]]))
    return matrix


def sine_coefficients():
    nodes = np.cos(np.pi * (np.arange(64) + 0.5) / 64)
    r2 = 0.125 + 0.125 * nodes
    root = np.sqrt(r2)
    target = np.sinc(2 * root)
    return np.polynomial.chebyshev.Chebyshev.fit(r2, target, 6, domain=[0, 0.25]).convert(
        kind=np.polynomial.Polynomial
    ).coef


SINE = [float(c) for c in sine_coefficients()]


def kernel(
    a_hbm, r_hbm, w_hbm, out,
    a_in, table, weight, mixed, gathered, rotated, quant, dequant,
    part, far, near, summed, far2, near2,
    in_sem, w_sem, send_a, recv_a, send_q, recv_q,
    send1, send2, recv_far, recv_near, recv_far2, recv_near2, heard,
):
    me = lax.axis_index("tensor")
    z, y = me // 4, me % 4
    width = a_hbm.shape[-1]
    half = width // 2
    norm = 1.0 / math.sqrt(width * 16)

    def partner(offset):
        return ((z + offset[0]) % 4) * 4 + (y + offset[1]) % 4

    loads = [
        pltpu.make_async_copy(a_hbm.at[:, pl.ds(ROWS * c, ROWS)], a_in.at[c], in_sem.at[c])
        for c in range(CHUNKS)
    ]
    table_load = pltpu.make_async_copy(r_hbm, table, in_sem.at[CHUNKS])
    loads[0].start()
    table_load.start()
    for c in range(1, CHUNKS):
        loads[c].start()
    w_loads = [
        pltpu.make_async_copy(w_hbm.at[:, pl.ds(WIDE * i, WIDE)], weight.at[i], w_sem.at[i])
        for i in range(2 * PIECES)
    ]

    barrier = pltpu.get_barrier_semaphore()
    for offset in OFFSETS[0]:
        pl.semaphore_signal(
            barrier, inc=1, device_id={"tensor": partner(offset)}, device_id_type=MESH
        )

    def hear(stage):
        pl.semaphore_wait(barrier if stage == 0 else heard.at[stage - 1], 4)
        if stage < 3:
            for offset in OFFSETS[0]:
                pl.semaphore_signal(
                    heard.at[stage], inc=1,
                    device_id={"tensor": partner(offset)}, device_id_type=MESH,
                )

    def rotate(c, places):
        rows = [a_in[c, e] for e in places]
        left = jnp.concatenate([row[:, 0:half] for row in rows], axis=0)
        right = jnp.concatenate([row[:, half:width] for row in rows], axis=0)
        for at in range(0, half, 256):
            size = min(256, half - at)
            cols = table[:, at : at + size]
            first = jnp.dot(left, cols, preferred_element_type=jnp.float32)
            second = jnp.dot(right, cols, preferred_element_type=jnp.float32)
            plus, minus = (first + second).astype(jnp.bfloat16), (first - second).astype(jnp.bfloat16)
            for i, e in enumerate(places):
                here = slice(i * ROWS, (i + 1) * ROWS)
                mixed[c, e, :, at : at + size] = plus[here]
                mixed[c, e, :, half + at : half + at + size] = minus[here]

    def exchange(c, stages, source, target, send, recv):
        for offset in sum((OFFSETS[stage] for stage in stages), ()):
            e = partner(offset)
            pltpu.make_async_remote_copy(
                src_ref=source.at[c, e],
                dst_ref=target.at[c, me],
                send_sem=send.at[c],
                recv_sem=recv.at[c],
                device_id={"tensor": e},
                device_id_type=MESH,
            ).start()

    def exchange_all(c, source, target, send, recv):
        return pltpu.make_async_remote_copy(
            src_ref=source.at[c, pl.ds(0, 15)],
            dst_ref=target.at[c, pl.ds(0, 15)],
            send_sem=send.at[c],
            recv_sem=recv.at[c],
            device_id={"tensor": partner((0, 1))},
            device_id_type=MESH,
        )

    def transform(c):
        def butterfly(t, largest):
            cols = pl.ds(pl.multiple_of(t * 128, 128), 128)
            v = [gathered[c, e, :, cols].astype(jnp.float32) for e in range(16)]
            for bit in (1, 2, 4, 8):
                n = list(v)
                for e in range(16):
                    n[e] = v[e ^ bit] - v[e] if e & bit else v[e] + v[e ^ bit]
                v = n
            for e in range(16):
                rotated[e, :, cols] = v[e]
            m = [jnp.abs(x) for x in v]
            while len(m) > 1:
                m = [jnp.maximum(m[i], m[i + 1]) for i in range(0, len(m), 2)]
            return jnp.maximum(largest, m[0])

        largest = lax.fori_loop(
            0, width // 128, butterfly, jnp.zeros((ROWS, 128), jnp.float32)
        )
        scale = jnp.maximum(jnp.max(largest, axis=1, keepdims=True) * norm, 1.0)
        up = jnp.broadcast_to(7.0 * norm / scale, (ROWS, 128))
        down = jnp.broadcast_to(scale / 7.0, (ROWS, 128))

        def staircase(t, carry):
            cols = pl.ds(pl.multiple_of(t * 128, 128), 128)
            for e in range(16):
                levels = rotated[e, :, cols] * up
                r = levels - jnp.round(levels)
                r2 = r * r
                series = jnp.full_like(r2, SINE[-1])
                for coefficient in SINE[-2::-1]:
                    series = series * r2 + coefficient
                quant[c, e, :, cols] = ((levels - r * series) * down).astype(jnp.bfloat16)
            return carry

        lax.fori_loop(0, width // 128, staircase, 0)

    def axes(h):
        along_y = [partner((0, 1)), partner((0, 3)), partner((0, 2))]
        along_z = [partner((1, 0)), partner((3, 0)), partner((2, 0))]
        return (y, z, along_y, along_z) if h == 0 else (z, y, along_z, along_y)

    def send(source, target, s, r, e):
        pltpu.make_async_remote_copy(
            src_ref=source, dst_ref=target, send_sem=s, recv_sem=r,
            device_id={"tensor": e}, device_id_type=MESH,
        ).start()

    order = [(c, p, h) for c in range(CHUNKS) for p in range(PIECES) for h in range(2)]

    def project(k):
        for g in (2 * k, 2 * k + 1):
            multiply(g)
        flows = [[], []]
        for h in range(2):
            g = 2 * k + h
            u, v, first, second = axes(h)
            up, down, opposite = (u + 1) % 4, (u + 3) % 4, (u + 2) % 4
            flows[h] = [
                (part.at[g, opposite, low], far.at[g, 0], send1.at[g], recv_far.at[g], first[0]),
                (part.at[g, opposite, high], far.at[g, 1], send1.at[g], recv_far.at[g], first[1]),
                (part.at[g, up, high], near.at[g, 0, high], send1.at[g], recv_near.at[g], first[0]),
                (part.at[g, down, low], near.at[g, 1, low], send1.at[g], recv_near.at[g], first[1]),
            ]
        interleave(flows)

    def interleave(flows):
        for pair in zip(*flows):
            for flow in pair:
                send(*flow)

    def multiply(g):
        c, p, h = order[g]
        i = h * PIECES + p
        if c == 0:
            w_loads[i].wait()

        product = jnp.dot(
            dequant[c].reshape(16 * ROWS, width), weight[i], preferred_element_type=jnp.float32
        ).astype(jnp.bfloat16)
        for e in range(16):
            u, v = (e % 4, e // 4) if h == 0 else (e // 4, e % 4)
            part[g, u, v] = product[e * ROWS : (e + 1) * ROWS]

    def fake(source, target, s, r):
        return pltpu.make_async_remote_copy(
            src_ref=source, dst_ref=target, send_sem=s, recv_sem=r,
            device_id={"tensor": partner((0, 1))}, device_id_type=MESH,
        )

    low, high = pl.ds(0, 2), pl.ds(2, 2)
    left, right = pl.ds(0, WIDE // 2), pl.ds(WIDE // 2, WIDE // 2)

    def relay(k):
        flows = [[], []]
        for h in range(2):
            g = 2 * k + h
            u, v, first, second = axes(h)
            up, down = (u + 1) % 4, (u + 3) % 4
            fake(far.at[g], far.at[g], send1.at[g], recv_far.at[g]).wait_recv()
            for j in range(2):
                part[g, up, j] = (
                    part[g, up, j].astype(jnp.float32) + far[g, 0, j].astype(jnp.float32)
                ).astype(jnp.bfloat16)
                part[g, down, 2 + j] = (
                    part[g, down, 2 + j].astype(jnp.float32) + far[g, 1, j].astype(jnp.float32)
                ).astype(jnp.bfloat16)
            flows[h] = [
                (part.at[g, up, low], near.at[g, 0, low], send1.at[g], recv_near.at[g], first[0]),
                (part.at[g, down, high], near.at[g, 1, high], send1.at[g], recv_near.at[g], first[1]),
            ]
        interleave(flows)

    def gather(k):
        flows = [[], []]
        for h in range(2):
            g = 2 * k + h
            u, v, first, second = axes(h)
            fake(near.at[g], near.at[g], send1.at[g], recv_near.at[g]).wait_recv()
            for j in range(4):
                summed[g, j] = (
                    part[g, u, j].astype(jnp.float32)
                    + near[g, 0, j].astype(jnp.float32)
                    + near[g, 1, j].astype(jnp.float32)
                ).astype(jnp.bfloat16)
            up, down, opposite = (v + 1) % 4, (v + 3) % 4, (v + 2) % 4
            if k in DIRECT:
                flows[h] = [
                    (summed.at[g, opposite], near2.at[g, 2], send2.at[g], recv_near2.at[g], second[2]),
                    (summed.at[g, up], near2.at[g, 0], send2.at[g], recv_near2.at[g], second[0]),
                    (summed.at[g, down], near2.at[g, 1], send2.at[g], recv_near2.at[g], second[1]),
                ]
                continue
            flows[h] = [
                (summed.at[g, opposite, :, left], far2.at[g, 0], send2.at[g], recv_far2.at[g], second[0]),
                (summed.at[g, opposite, :, right], far2.at[g, 1], send2.at[g], recv_far2.at[g], second[1]),
                (summed.at[g, up, :, right], near2.at[g, 0, :, right], send2.at[g], recv_near2.at[g], second[0]),
                (summed.at[g, down, :, left], near2.at[g, 1, :, left], send2.at[g], recv_near2.at[g], second[1]),
            ]
        interleave(flows)

    def relay2(k):
        if k in DIRECT:
            return
        flows = [[], []]
        for h in range(2):
            g = 2 * k + h
            u, v, first, second = axes(h)
            up, down = (v + 1) % 4, (v + 3) % 4
            fake(far2.at[g], far2.at[g], send2.at[g], recv_far2.at[g]).wait_recv()
            summed[g, up, :, left] = (
                summed[g, up, :, left].astype(jnp.float32) + far2[g, 0].astype(jnp.float32)
            ).astype(jnp.bfloat16)
            summed[g, down, :, right] = (
                summed[g, down, :, right].astype(jnp.float32) + far2[g, 1].astype(jnp.float32)
            ).astype(jnp.bfloat16)
            flows[h] = [
                (summed.at[g, up, :, left], near2.at[g, 0, :, left], send2.at[g], recv_near2.at[g], second[0]),
                (summed.at[g, down, :, right], near2.at[g, 1, :, right], send2.at[g], recv_near2.at[g], second[1]),
            ]
        interleave(flows)

    def finish(k):
        for h in range(2):
            g = 2 * k + h
            c, p, _ = order[g]
            u, v, first, second = axes(h)
            count = 3 if k in DIRECT else 2
            landed = near2.at[g, pl.ds(0, count)]
            fake(landed, landed, send2.at[g], recv_near2.at[g]).wait_recv()
            total = summed[g, v].astype(jnp.float32)
            for j in range(count):
                total = total + near2[g, j].astype(jnp.float32)
            at = (h * PIECES + p) * WIDE
            out[c * ROWS : (c + 1) * ROWS, at : at + WIDE] = total.astype(jnp.bfloat16)

    hear(0)
    table_load.wait()
    loads[0].wait()
    for stage in range(4):
        if stage < 2:
            rotate(0, [partner(o) for o in OFFSETS[stage]])
        if stage == 2:
            rotate(0, [partner(o) for o in OFFSETS[2] + OFFSETS[3]] + [me])
        if stage > 0:
            hear(stage)
        exchange(0, (stage,), mixed, gathered, send_a, recv_a)
    loads[1].wait()
    rotate(1, list(range(16)))
    exchange(1, range(4), mixed, gathered, send_a, recv_a)
    for load in w_loads:
        load.start()
    for c in range(CHUNKS):
        gathered[c, me] = mixed[c, me]
        exchange_all(c, mixed, gathered, send_a, recv_a).wait_recv()
        transform(c)
        exchange(c, range(4), quant, dequant, send_q, recv_q)
        dequant[c, me] = quant[c, me]
    each = PIECES
    exchange_all(0, quant, dequant, send_q, recv_q).wait_recv()
    for g in range(each):
        project(g)
    exchange_all(1, quant, dequant, send_q, recv_q).wait_recv()
    for g in range(each):
        project(each + g)
        relay(g)
    for g in range(each):
        relay(each + g)
        gather(g)
    relay2(0)
    gather(each)
    relay2(1)
    gather(each + 1)
    gather(each + 2)
    relay2(2)
    for g in range(each):
        finish(g)
    for g in range(each):
        finish(each + g)

    for c in range(CHUNKS):
        exchange_all(c, mixed, gathered, send_a, recv_a).wait_send()
        exchange_all(c, quant, dequant, send_q, recv_q).wait_send()
    for g in range(len(order)):
        fake(part.at[g, pl.ds(0, 3)], part.at[g, pl.ds(0, 3)], send1.at[g], recv_far.at[g]).wait_send()
        fake(summed.at[g, pl.ds(0, 3)], summed.at[g, pl.ds(0, 3)], send2.at[g], recv_far2.at[g]).wait_send()


def shards(activations, down_weight):
    count_rows, width = activations.shape
    features = down_weight.shape[1]
    table = jnp.asarray(np.kron(sylvester(32), paley_matrix()), jnp.bfloat16)
    bf16, f32 = jnp.bfloat16, jnp.float32
    groups = CHUNKS * PIECES * 2
    dma = pltpu.SemaphoreType.DMA
    return pl.pallas_call(
        kernel,
        out_shape=jax.ShapeDtypeStruct((count_rows // 16, features), bf16),
        in_specs=[pl.BlockSpec(memory_space=pltpu.HBM)] * 3,
        out_specs=pl.BlockSpec(memory_space=pltpu.VMEM),
        scratch_shapes=[
            pltpu.VMEM((CHUNKS, 16, ROWS, width), bf16),
            pltpu.VMEM(table.shape, bf16),
            pltpu.VMEM((2 * PIECES, width, WIDE), bf16),
            pltpu.VMEM((CHUNKS, 16, ROWS, width), bf16),
            pltpu.VMEM((CHUNKS, 16, ROWS, width), bf16),
            pltpu.VMEM((16, ROWS, width), f32),
            pltpu.VMEM((CHUNKS, 16, ROWS, width), bf16),
            pltpu.VMEM((CHUNKS, 16, ROWS, width), bf16),
            pltpu.VMEM((groups, 4, 4, ROWS, WIDE), bf16),
            pltpu.VMEM((groups, 2, 2, ROWS, WIDE), bf16),
            pltpu.VMEM((groups, 2, 4, ROWS, WIDE), bf16),
            pltpu.VMEM((groups, 4, ROWS, WIDE), bf16),
            pltpu.VMEM((groups, 2, ROWS, WIDE // 2), bf16),
            pltpu.VMEM((groups, 3, ROWS, WIDE), bf16),
            dma((CHUNKS + 1,)),
            dma((2 * PIECES,)),
            dma((CHUNKS,)), dma((CHUNKS,)), dma((CHUNKS,)), dma((CHUNKS,)),
            dma((groups,)), dma((groups,)),
            dma((groups,)), dma((groups,)), dma((groups,)), dma((groups,)),
            pltpu.SemaphoreType.REGULAR((3,)),
        ],
        compiler_params=pltpu.CompilerParams(
            collective_id=0, has_side_effects=True, vmem_limit_bytes=53 * 2**20
        ),
        name="rotate_quantize_project",
    )(activations.reshape(16, count_rows // 16, width), table, down_weight)


def solution(mesh):
    placed = (P("dp", "tensor"), P("tensor", None))
    return jax.shard_map(
        shards, mesh=mesh, in_specs=placed, out_specs=P(("dp", "tensor"), None), check_vma=False
    )
```

```python
import functools
import math

import jax
import jax.numpy as jnp
import numpy as np
from jax import lax
from jax.experimental import pallas as pl
from jax.experimental.pallas import tpu as pltpu
from jax.sharding import PartitionSpec as P

MESH = pl.DeviceIdType.MESH
CHUNKS = 2
ROWS = 16
PIECES = 3
WIDE = 1024
DIRECT = (2, 3, 4, 5)
OFFSETS = (
    ((0, 1), (1, 0), (0, 3), (3, 0)),
    ((1, 1), (3, 3), (1, 3), (3, 1), (0, 2), (2, 0)),
    ((1, 2), (2, 1), (3, 2), (2, 3)),
    ((2, 2),),
)


def paley_matrix():
    modulus = 13
    residues = set((value * value % modulus for value in range(1, modulus)))
    confer = np.zeros((14, 14))
    confer[0, 1:] = 1.0
    confer[1:, 0] = 1.0
    for row in range(modulus):
        for col in range(modulus):
            if row != col:
                confer[1 + row, 1 + col] = 1.0 if (col - row) % modulus in residues else -1.0
    return np.kron(confer, np.array([[1.0, 1.0], [1.0, -1.0]])) + np.kron(
        np.eye(14), np.array([[1.0, -1.0], [-1.0, -1.0]])
    )


def sylvester(order):
    matrix = np.ones((1, 1))
    while matrix.shape[0] < order:
        matrix = np.kron(matrix, np.array([[1.0, 1.0], [1.0, -1.0]]))
    return matrix


def sine_coefficients():
    nodes = np.cos(np.pi * (np.arange(64) + 0.5) / 64)
    r2 = 0.125 + 0.125 * nodes
    root = np.sqrt(r2)
    target = np.sinc(2 * root)
    return np.polynomial.chebyshev.Chebyshev.fit(r2, target, 6, domain=[0, 0.25]).convert(
        kind=np.polynomial.Polynomial
    ).coef


SINE = [float(c) for c in sine_coefficients()]


def kernel(
    a_hbm, r_hbm, w_hbm, out,
    a_in, table, weight, mixed, gathered, rotated, quant, dequant,
    part, far, near, summed, far2, near2,
    in_sem, w_sem, send_a, recv_a, send_q, recv_q,
    send1, send2, recv_far, recv_near, recv_far2, recv_near2, heard,
):
    me = lax.axis_index("tensor")
    z, y = me // 4, me % 4
    width = a_hbm.shape[-1]
    half = width // 2
    norm = 1.0 / math.sqrt(width * 16)

    def partner(offset):
        return ((z + offset[0]) % 4) * 4 + (y + offset[1]) % 4

    loads = [
        pltpu.make_async_copy(a_hbm.at[:, pl.ds(ROWS * c, ROWS)], a_in.at[c], in_sem.at[c])
        for c in range(CHUNKS)
    ]
    table_load = pltpu.make_async_copy(r_hbm, table, in_sem.at[CHUNKS])
    loads[0].start()
    table_load.start()
    for c in range(1, CHUNKS):
        loads[c].start()
    w_loads = [
        pltpu.make_async_copy(w_hbm.at[:, pl.ds(WIDE * i, WIDE)], weight.at[i], w_sem.at[i])
        for i in range(2 * PIECES)
    ]

    barrier = pltpu.get_barrier_semaphore()
    for offset in OFFSETS[0]:
        pl.semaphore_signal(
            barrier, inc=1, device_id={"tensor": partner(offset)}, device_id_type=MESH
        )

    def hear(stage):
        pl.semaphore_wait(barrier if stage == 0 else heard.at[stage - 1], 4)
        if stage < 3:
            for offset in OFFSETS[0]:
                pl.semaphore_signal(
                    heard.at[stage], inc=1,
                    device_id={"tensor": partner(offset)}, device_id_type=MESH,
                )

    def rotate(c, places):
        rows = [a_in[c, e] for e in places]
        left = jnp.concatenate([row[:, 0:half] for row in rows], axis=0)
        right = jnp.concatenate([row[:, half:width] for row in rows], axis=0)
        for at in range(0, half, 256):
            size = min(256, half - at)
            cols = table[:, at : at + size]
            first = jnp.dot(left, cols, preferred_element_type=jnp.float32)
            second = jnp.dot(right, cols, preferred_element_type=jnp.float32)
            plus, minus = (first + second).astype(jnp.bfloat16), (first - second).astype(jnp.bfloat16)
            for i, e in enumerate(places):
                here = slice(i * ROWS, (i + 1) * ROWS)
                mixed[c, e, :, at : at + size] = plus[here]
                mixed[c, e, :, half + at : half + at + size] = minus[here]

    def exchange(c, stages, source, target, send, recv):
        for offset in sum((OFFSETS[stage] for stage in stages), ()):
            e = partner(offset)
            pltpu.make_async_remote_copy(
                src_ref=source.at[c, e],
                dst_ref=target.at[c, me],
                send_sem=send.at[c],
                recv_sem=recv.at[c],
                device_id={"tensor": e},
                device_id_type=MESH,
            ).start()

    def exchange_all(c, source, target, send, recv):
        return pltpu.make_async_remote_copy(
            src_ref=source.at[c, pl.ds(0, 15)],
            dst_ref=target.at[c, pl.ds(0, 15)],
            send_sem=send.at[c],
            recv_sem=recv.at[c],
            device_id={"tensor": partner((0, 1))},
            device_id_type=MESH,
        )

    def transform(c):
        def butterfly(t, largest):
            cols = pl.ds(pl.multiple_of(t * 128, 128), 128)
            v = [gathered[c, e, :, cols].astype(jnp.float32) for e in range(16)]
            for bit in (1, 2, 4, 8):
                n = list(v)
                for e in range(16):
                    n[e] = v[e ^ bit] - v[e] if e & bit else v[e] + v[e ^ bit]
                v = n
            for e in range(16):
                rotated[e, :, cols] = v[e]
            m = [jnp.abs(x) for x in v]
            while len(m) > 1:
                m = [jnp.maximum(m[i], m[i + 1]) for i in range(0, len(m), 2)]
            return jnp.maximum(largest, m[0])

        largest = lax.fori_loop(
            0, width // 128, butterfly, jnp.zeros((ROWS, 128), jnp.float32)
        )
        scale = jnp.maximum(jnp.max(largest, axis=1, keepdims=True) * norm, 1.0)
        up = jnp.broadcast_to(7.0 * norm / scale, (ROWS, 128))
        down = jnp.broadcast_to(scale / 7.0, (ROWS, 128))

        def staircase(t, carry):
            cols = pl.ds(pl.multiple_of(t * 128, 128), 128)
            for e in range(16):
                levels = rotated[e, :, cols] * up
                r = levels - jnp.round(levels)
                r2 = r * r
                series = jnp.full_like(r2, SINE[-1])
                for coefficient in SINE[-2::-1]:
                    series = series * r2 + coefficient
                quant[c, e, :, cols] = ((levels - r * series) * down).astype(jnp.bfloat16)
            return carry

        lax.fori_loop(0, width // 128, staircase, 0)

    def axes(h):
        along_y = [partner((0, 1)), partner((0, 3)), partner((0, 2))]
        along_z = [partner((1, 0)), partner((3, 0)), partner((2, 0))]
        return (y, z, along_y, along_z) if h == 0 else (z, y, along_z, along_y)

    def send(source, target, s, r, e):
        pltpu.make_async_remote_copy(
            src_ref=source, dst_ref=target, send_sem=s, recv_sem=r,
            device_id={"tensor": e}, device_id_type=MESH,
        ).start()

    order = [(c, p, h) for c in range(CHUNKS) for p in range(PIECES) for h in range(2)]

    def project(k):
        for g in (2 * k, 2 * k + 1):
            multiply(g)
        flows = [[], []]
        for h in range(2):
            g = 2 * k + h
            u, v, first, second = axes(h)
            up, down, opposite = (u + 1) % 4, (u + 3) % 4, (u + 2) % 4
            flows[h] = [
                (part.at[g, opposite, low], far.at[g, 0], send1.at[g], recv_far.at[g], first[0]),
                (part.at[g, opposite, high], far.at[g, 1], send1.at[g], recv_far.at[g], first[1]),
                (part.at[g, up, high], near.at[g, 0, high], send1.at[g], recv_near.at[g], first[0]),
                (part.at[g, down, low], near.at[g, 1, low], send1.at[g], recv_near.at[g], first[1]),
            ]
        interleave(flows)

    def interleave(flows):
        for pair in zip(*flows):
            for flow in pair:
                send(*flow)

    def multiply(g):
        c, p, h = order[g]
        i = h * PIECES + p
        if c == 0:
            w_loads[i].wait()

        product = jnp.dot(
            dequant[c].reshape(16 * ROWS, width), weight[i], preferred_element_type=jnp.float32
        ).astype(jnp.bfloat16)
        for e in range(16):
            u, v = (e % 4, e // 4) if h == 0 else (e // 4, e % 4)
            part[g, u, v] = product[e * ROWS : (e + 1) * ROWS]

    def fake(source, target, s, r):
        return pltpu.make_async_remote_copy(
            src_ref=source, dst_ref=target, send_sem=s, recv_sem=r,
            device_id={"tensor": partner((0, 1))}, device_id_type=MESH,
        )

    low, high = pl.ds(0, 2), pl.ds(2, 2)
    left, right = pl.ds(0, WIDE // 2), pl.ds(WIDE // 2, WIDE // 2)

    def relay(k):
        flows = [[], []]
        for h in range(2):
            g = 2 * k + h
            u, v, first, second = axes(h)
            up, down = (u + 1) % 4, (u + 3) % 4
            fake(far.at[g], far.at[g], send1.at[g], recv_far.at[g]).wait_recv()
            for j in range(2):
                part[g, up, j] = (
                    part[g, up, j].astype(jnp.float32) + far[g, 0, j].astype(jnp.float32)
                ).astype(jnp.bfloat16)
                part[g, down, 2 + j] = (
                    part[g, down, 2 + j].astype(jnp.float32) + far[g, 1, j].astype(jnp.float32)
                ).astype(jnp.bfloat16)
            flows[h] = [
                (part.at[g, up, low], near.at[g, 0, low], send1.at[g], recv_near.at[g], first[0]),
                (part.at[g, down, high], near.at[g, 1, high], send1.at[g], recv_near.at[g], first[1]),
            ]
        interleave(flows)

    def gather(k):
        flows = [[], []]
        for h in range(2):
            g = 2 * k + h
            u, v, first, second = axes(h)
            fake(near.at[g], near.at[g], send1.at[g], recv_near.at[g]).wait_recv()
            for j in range(4):
                summed[g, j] = (
                    part[g, u, j].astype(jnp.float32)
                    + near[g, 0, j].astype(jnp.float32)
                    + near[g, 1, j].astype(jnp.float32)
                ).astype(jnp.bfloat16)
            up, down, opposite = (v + 1) % 4, (v + 3) % 4, (v + 2) % 4
            if k in DIRECT:
                flows[h] = [
                    (summed.at[g, opposite], near2.at[g, 2], send2.at[g], recv_near2.at[g], second[2]),
                    (summed.at[g, up], near2.at[g, 0], send2.at[g], recv_near2.at[g], second[0]),
                    (summed.at[g, down], near2.at[g, 1], send2.at[g], recv_near2.at[g], second[1]),
                ]
                continue
            flows[h] = [
                (summed.at[g, opposite, :, left], far2.at[g, 0], send2.at[g], recv_far2.at[g], second[0]),
                (summed.at[g, opposite, :, right], far2.at[g, 1], send2.at[g], recv_far2.at[g], second[1]),
                (summed.at[g, up, :, right], near2.at[g, 0, :, right], send2.at[g], recv_near2.at[g], second[0]),
                (summed.at[g, down, :, left], near2.at[g, 1, :, left], send2.at[g], recv_near2.at[g], second[1]),
            ]
        interleave(flows)

    def relay2(k):
        if k in DIRECT:
            return
        flows = [[], []]
        for h in range(2):
            g = 2 * k + h
            u, v, first, second = axes(h)
            up, down = (v + 1) % 4, (v + 3) % 4
            fake(far2.at[g], far2.at[g], send2.at[g], recv_far2.at[g]).wait_recv()
            summed[g, up, :, left] = (
                summed[g, up, :, left].astype(jnp.float32) + far2[g, 0].astype(jnp.float32)
            ).astype(jnp.bfloat16)
            summed[g, down, :, right] = (
                summed[g, down, :, right].astype(jnp.float32) + far2[g, 1].astype(jnp.float32)
            ).astype(jnp.bfloat16)
            flows[h] = [
                (summed.at[g, up, :, left], near2.at[g, 0, :, left], send2.at[g], recv_near2.at[g], second[0]),
                (summed.at[g, down, :, right], near2.at[g, 1, :, right], send2.at[g], recv_near2.at[g], second[1]),
            ]
        interleave(flows)

    def finish(k):
        for h in range(2):
            g = 2 * k + h
            c, p, _ = order[g]
            u, v, first, second = axes(h)
            count = 3 if k in DIRECT else 2
            landed = near2.at[g, pl.ds(0, count)]
            fake(landed, landed, send2.at[g], recv_near2.at[g]).wait_recv()
            total = summed[g, v].astype(jnp.float32)
            for j in range(count):
                total = total + near2[g, j].astype(jnp.float32)
            at = (h * PIECES + p) * WIDE
            out[c * ROWS : (c + 1) * ROWS, at : at + WIDE] = total.astype(jnp.bfloat16)

    hear(0)
    table_load.wait()
    loads[0].wait()
    for stage in range(4):
        if stage < 2:
            rotate(0, [partner(o) for o in OFFSETS[stage]])
        if stage == 2:
            rotate(0, [partner(o) for o in OFFSETS[2] + OFFSETS[3]] + [me])
        if stage > 0:
            hear(stage)
        exchange(0, (stage,), mixed, gathered, send_a, recv_a)
    loads[1].wait()
    rotate(1, list(range(16)))
    exchange(1, range(4), mixed, gathered, send_a, recv_a)
    for load in w_loads:
        load.start()
    for c in range(CHUNKS):
        gathered[c, me] = mixed[c, me]
        exchange_all(c, mixed, gathered, send_a, recv_a).wait_recv()
        transform(c)
        exchange(c, range(4), quant, dequant, send_q, recv_q)
        dequant[c, me] = quant[c, me]
    each = PIECES
    exchange_all(0, quant, dequant, send_q, recv_q).wait_recv()
    for g in range(each):
        project(g)
    exchange_all(1, quant, dequant, send_q, recv_q).wait_recv()
    for g in range(each):
        project(each + g)
        relay(g)
    for g in range(each):
        relay(each + g)
        gather(g)
    for g in range(each):
        relay2(g)
        gather(each + g)
    for g in range(each):
        finish(g)
        relay2(each + g)
    for g in range(each):
        finish(each + g)

    for c in range(CHUNKS):
        exchange_all(c, mixed, gathered, send_a, recv_a).wait_send()
        exchange_all(c, quant, dequant, send_q, recv_q).wait_send()
    for g in range(len(order)):
        fake(part.at[g, pl.ds(0, 3)], part.at[g, pl.ds(0, 3)], send1.at[g], recv_far.at[g]).wait_send()
        fake(summed.at[g, pl.ds(0, 3)], summed.at[g, pl.ds(0, 3)], send2.at[g], recv_far2.at[g]).wait_send()


def shards(activations, down_weight):
    count_rows, width = activations.shape
    features = down_weight.shape[1]
    table = jnp.asarray(np.kron(sylvester(32), paley_matrix()), jnp.bfloat16)
    bf16, f32 = jnp.bfloat16, jnp.float32
    groups = CHUNKS * PIECES * 2
    dma = pltpu.SemaphoreType.DMA
    return pl.pallas_call(
        kernel,
        out_shape=jax.ShapeDtypeStruct((count_rows // 16, features), bf16),
        in_specs=[pl.BlockSpec(memory_space=pltpu.HBM)] * 3,
        out_specs=pl.BlockSpec(memory_space=pltpu.VMEM),
        scratch_shapes=[
            pltpu.VMEM((CHUNKS, 16, ROWS, width), bf16),
            pltpu.VMEM(table.shape, bf16),
            pltpu.VMEM((2 * PIECES, width, WIDE), bf16),
            pltpu.VMEM((CHUNKS, 16, ROWS, width), bf16),
            pltpu.VMEM((CHUNKS, 16, ROWS, width), bf16),
            pltpu.VMEM((16, ROWS, width), f32),
            pltpu.VMEM((CHUNKS, 16, ROWS, width), bf16),
            pltpu.VMEM((CHUNKS, 16, ROWS, width), bf16),
            pltpu.VMEM((groups, 4, 4, ROWS, WIDE), bf16),
            pltpu.VMEM((groups, 2, 2, ROWS, WIDE), bf16),
            pltpu.VMEM((groups, 2, 4, ROWS, WIDE), bf16),
            pltpu.VMEM((groups, 4, ROWS, WIDE), bf16),
            pltpu.VMEM((groups, 2, ROWS, WIDE // 2), bf16),
            pltpu.VMEM((groups, 3, ROWS, WIDE), bf16),
            dma((CHUNKS + 1,)),
            dma((2 * PIECES,)),
            dma((CHUNKS,)), dma((CHUNKS,)), dma((CHUNKS,)), dma((CHUNKS,)),
            dma((groups,)), dma((groups,)),
            dma((groups,)), dma((groups,)), dma((groups,)), dma((groups,)),
            pltpu.SemaphoreType.REGULAR((3,)),
        ],
        compiler_params=pltpu.CompilerParams(
            collective_id=0, has_side_effects=True, vmem_limit_bytes=53 * 2**20
        ),
        name="rotate_quantize_project",
    )(activations.reshape(16, count_rows // 16, width), table, down_weight)


def solution(mesh):
    placed = (P("dp", "tensor"), P("tensor", None))
    return jax.shard_map(
        shards, mesh=mesh, in_specs=placed, out_specs=P(("dp", "tensor"), None), check_vma=False
    )
```
